32 devices in a mesh: dp: 16 (over z, y, x), tensor: 2 (over core).
Axes of the slice: x: 2, y: 2, z: 4, core: 2. Of those that a mesh axis runs over, the one named last changes fastest.
Arguments:
- encoded: bfloat16 [8192, 1152], P('dp', 'tensor'), may hold values from -9 to 9
- counts: int32 [128], P('dp'), may hold values from 16 to 64
- win_ids: int32 [128, 64], P('dp'), may hold values from 0 to 31, never falling along the last dimension, each value on 1 to 8 neighbouring positions
- dest_seq: int32 [128], P('dp'), may hold values from 0 to 15, as said below
- dest_slot: int32 [128], P('dp'), may hold values from 0 to 7, as said below
- w_first: bfloat16 [1152, 4608], P(None, 'tensor'), may hold values from -0.3125 to 0.3125
- b_first: float32 [4608], P('tensor'), may hold values from -3 to 3
- w_second: bfloat16 [4608, 2304], P('tensor'), may hold values from -0.1875 to 0.1875
- b_second: float32 [2304], P('tensor'), may hold values from -3 to 3
Outputs:
- projected: bfloat16 [4096, 2304], P('dp', 'tensor')
The draws below stay inside these ranges and needn't reach their ends.
Inputs may be any that keep to these rules, and one draw needn't show every extreme that they name: `dest_seq`: every sequence receives exactly 8 samples, no two of them from the same index of dp. `dest_slot`: the samples that one sequence receives have distinct block offsets.
All inputs are finite; a program needn't handle non-finite values.
Results may differ from the reference program's by a relative error of at most 0.009.
Values may be sent and summed in bfloat16 or wider, within the bound.
A program may use at most 128 MiB of HBM per device.

```python
import math
import jax
import jax.numpy as jnp
import numpy as np
from jax import lax

F = 1152
H = 4608
E = 2304
CAP = 64
BLOCK = 32
MOST = 8
SAMP_DEV = 8
SAMPLES = 128
N_TENSOR = 2


def routing_tables(key):
    base = jax.random.fold_in(key, 11)
    key_outer, key_inner, key_shift, key_slots = jax.random.split(base, 4)
    groups = SAMPLES // SAMP_DEV
    outer_perm = jax.random.permutation(key_outer, groups)
    inner_perm = jax.random.permutation(key_inner, groups)
    shifts = jax.random.permutation(key_shift, groups)[:SAMP_DEV]
    sequence = outer_perm[(inner_perm[:, None] + shifts[None, :]) % groups]
    slot_table = jax.vmap(lambda single: jax.random.permutation(single, SAMP_DEV))(jax.random.split(key_slots, groups))
    slot_ids = slot_table[sequence, jnp.arange(SAMP_DEV)[None, :]]
    return (sequence.reshape(-1).astype(jnp.int32), slot_ids.reshape(-1).astype(jnp.int32))


def draw_dest_seq(key, part):
    return routing_tables(key)[0]


def draw_dest_slot(key, part):
    return routing_tables(key)[1]


def touch_ends(array, rng, least, largest):
    spot = [jax.random.randint(jax.random.fold_in(rng, axis), (), 0, length) for axis, length in enumerate(array.shape)]
    longest = array.shape.index(max(array.shape))
    beside = spot[:longest] + [(spot[longest] + 1) % array.shape[longest]] + spot[longest + 1:]
    return array.at[tuple(spot)].set(least).at[tuple(beside)].set(largest)


def with_spikes(result, stream_key, source, target, blocks, factor):
    owner, partner = [(jnp.arange(result.shape[dim]) // (result.shape[dim] // blocks)).reshape([-1 if axis == dim else 1 for axis in range(result.ndim)]) for dim in (source, target)]
    chosen = jax.random.permutation(stream_key, blocks)[partner]
    strong = (owner == chosen) | (owner == (partner + blocks // 2) % blocks)
    return jnp.where(strong, factor * result, result)


def shard_levels(key, dims, pieces, low, top_value):
    loudness = 1.0
    for dim, blocks in pieces:
        heights = jax.random.uniform(jax.random.fold_in(jax.random.fold_in(key, 6), dim), (blocks,), jnp.float32, low / len(pieces), top_value / len(pieces))
        loudness = loudness * jnp.repeat(jnp.exp(heights), dims[dim] // blocks).reshape((-1,) + (1,) * (len(dims) - 1 - dim))
    return loudness


def length_profile(count, total, most, lean):
    portions = [(1 << 20) // math.isqrt(rank ** lean) + 1 for rank in range(2, count + 1)]
    rest, given = total - most - (count - 1), [1] * (count - 1)
    while rest > 0:
        free = [i for i in range(count - 1) if given[i] < most]
        mass, remaining = sum([portions[i] for i in free]), rest
        for i in free:
            more = min(most - given[i], max(1, remaining * portions[i] // mass), rest)
            given[i] = given[i] + more
            rest = rest - more
    return np.array([most] + given)


def uneven(key, count, total, most, lean):
    if count == 2:
        one = jax.random.randint(key, (), max(1, total - most), min(most, total - 1) + 1)
        return jnp.stack([one, total - one])
    sizes = jnp.asarray(length_profile(count, total, most, lean), jnp.int32)
    pairs = (count - 1) // 2
    donor, sink = sizes[1:1 + 2 * pairs:2], sizes[2:2 + 2 * pairs:2]
    margin = jnp.minimum(donor - 1, most - sink)
    shifted = jax.random.randint(jax.random.fold_in(key, 1), (pairs,), 0, 1 << 20) % (margin + 1)
    sizes = sizes.at[1:1 + 2 * pairs:2].set(donor - shifted).at[2:2 + 2 * pairs:2].set(sink + shifted)
    return sizes[jax.random.permutation(jax.random.fold_in(key, 2), count)]


def bell_draw(own_key, shape, scale, reach, cuts=(), kind=jnp.bfloat16):
    loudness = shard_levels(own_key, shape, cuts, -0.22, 0.18) if cuts else 1.0
    drawn = jax.random.normal(own_key, shape, jnp.float32) * scale * loudness
    return jnp.minimum(jnp.maximum(drawn, -reach), reach).astype(kind)


def heavy_noise(rng, shape, spread, bound, cuts, heavy, held_as=jnp.bfloat16):
    drawn = spread * jax.random.normal(rng, shape, jnp.float32)
    if cuts:
        drawn = drawn * shard_levels(rng, shape, cuts, -0.22, 0.18)
    return jnp.clip(with_spikes(drawn, jax.random.fold_in(rng, 3), *heavy), -bound, bound).astype(held_as)


def setup_inputs(seed: int = 0) -> dict:
    streams_of = jax.random.split(jax.random.key(seed), 10)
    return {
        "encoded": bell_draw(streams_of[0], (SAMPLES * CAP, F), 1.5, 9.0, ((0, 16), (1, 2))),
        "counts": touch_ends(jax.random.randint(streams_of[1], (SAMPLES,), CAP // 4, CAP + 1), jax.random.fold_in(streams_of[1], 1), CAP // 4, CAP).astype(jnp.int32),
        "win_ids": jax.vmap(lambda own: jnp.searchsorted(jnp.cumsum(uneven(own, BLOCK, CAP, MOST, 1)), jnp.arange(CAP), side="right"))(jax.random.split(streams_of[2], SAMPLES)).reshape((SAMPLES, CAP)).astype(jnp.int32),
        "dest_seq": draw_dest_seq(jax.random.fold_in(streams_of[9], 71), 0),
        "dest_slot": draw_dest_slot(jax.random.fold_in(streams_of[9], 71), 0),
        "w_first": bell_draw(streams_of[5], (F, H), (F // 3) ** -0.5, 0.3125, ((1, 2),)),
        "b_first": bell_draw(streams_of[6], (H,), 0.5, 3.0, ((0, 2),), jnp.float32),
        "w_second": heavy_noise(streams_of[7], (H, E), (H // 2) ** -0.5, 0.1875, ((0, 2),), (0, 1, 2, 2.0)),
        "b_second": bell_draw(streams_of[8], (E,), 0.5, 3.0, ((0, 2),), jnp.float32),
    }


def reference(encoded, counts, win_ids, dest_seq, dest_slot, w_first, b_first, w_second, b_second):
    tokens = encoded.reshape(SAMPLES, CAP, F)
    positions = jnp.arange(CAP, dtype=jnp.int32)
    ids_live = jnp.where(positions[None, :] < counts[:, None], win_ids, -1)
    windows = jnp.arange(BLOCK, dtype=jnp.int32)
    onehot = (ids_live[:, None, :] == windows[None, :, None]).astype(jnp.float32)
    number = jnp.sum(onehot, axis=2)
    totals = jnp.einsum("nwc,ncf->nwf", onehot, tokens.astype(jnp.float32))
    pooled = (totals / jnp.maximum(number, 1.0)[:, :, None]).astype(jnp.bfloat16)
    position = (dest_seq * SAMP_DEV + dest_slot).astype(jnp.int32)
    packed = jnp.zeros((SAMPLES, BLOCK, F), jnp.bfloat16).at[position].set(pooled)
    packed = packed.reshape(SAMPLES * BLOCK, F)
    preact = jnp.dot(packed, w_first, preferred_element_type=jnp.float32) + b_first
    hidden = jax.nn.gelu(preact, approximate=True).astype(jnp.bfloat16)
    quota_size = H // N_TENSOR
    running = jnp.zeros((SAMPLES * BLOCK, E), jnp.float32)
    for member in range(N_TENSOR):
        portion = jnp.dot(hidden[:, member * quota_size:(member + 1) * quota_size],
                          w_second[member * quota_size:(member + 1) * quota_size],
                          preferred_element_type=jnp.float32).astype(jnp.bfloat16)
        portion = lax.optimization_barrier(portion)
        running = running + portion.astype(jnp.float32)
    return (running + b_second).astype(jnp.bfloat16)
```

```python
import functools
import math

import jax
import jax.numpy as jnp
from jax import lax
from jax.experimental import pallas as pl
from jax.experimental.pallas import tpu as pltpu
from jax.sharding import PartitionSpec as P

BLOCK = 32
LANES = 128
MESH = pl.DeviceIdType.MESH
UNROLL_MAX = 16


def loop(count, body):
    if count <= UNROLL_MAX:
        for i in range(count):
            body(i)
    else:

        @pl.loop(0, count)
        def _(i):
            body(i)


def col_chunks(width, step):
    return [(lo, min(step, width - lo)) for lo in range(0, width, step)]


def gelu(x):
    c0 = math.sqrt(2.0 / math.pi)
    half = 0.5 * x
    return half + half * jnp.tanh(x * (c0 + (c0 * 0.044715) * (x * x)))


def kernel(
    dims,
    seq_h, slot_h, cnt_h, win_h, b1_h, b2_h, enc_h, w1_h, w2_h,
    out_v,
    seq_s, slot_s, cnt_s, win_v, b1_v, b2_v, enc, w1, w2, pooled, outgo, arr, sib, route_src, routes, xbuf, hidden, part_out, part_in,
    small_sem, load_sem, w1_sem, w2_sem, send_sem, recv_sem, rsend_sem, rrecv_sem, fsend_sem, frecv_sem,
    psend_sem, precv_sem,
):
    groups, samples, cap, feat = dims
    full = feat // LANES
    rem = feat - full * LANES
    me = lax.axis_index("dp")
    core = lax.axis_index("tensor")
    other = 1 - core

    barrier = pltpu.get_barrier_semaphore()
    pl.semaphore_signal(barrier, 1, device_id={"tensor": other}, device_id_type=MESH)

    def greet(i):
        peer = lax.rem(me + 1 + i, groups)
        pl.semaphore_signal(barrier, 1, device_id={"dp": peer}, device_id_type=MESH)

    loop(groups - 1, greet)

    pairs = enc.shape[0]
    enc_copies = [
        pltpu.make_async_copy(enc_h.at[:, p * LANES : (p + 1) * LANES], enc.at[p], load_sem.at[p])
        for p in range(pairs)
    ]
    for copy in enc_copies:
        copy.start()
    small = [
        pltpu.make_async_copy(src, dst, small_sem.at[n])
        for n, (src, dst) in enumerate(
            [(seq_h, seq_s), (slot_h, slot_s), (cnt_h, cnt_s), (win_h, win_v), (b1_h, b1_v), (b2_h, b2_v)]
        )
    ]
    for copy in small:
        copy.start()

    wide = full * LANES
    mine = pl.multiple_of(core * feat, 64)
    theirs = pl.multiple_of(other * feat, 64)
    spans = [(mine, 0, wide), (theirs, wide, wide)]
    if rem:
        spans += [
            (pl.multiple_of(core * feat + wide, 64), 2 * wide, rem),
            (pl.multiple_of(other * feat + wide, 64), 2 * wide + rem, rem),
        ]
    w1_copies = [
        pltpu.make_async_copy(w1_h.at[pl.ds(src, size)], w1.at[pl.ds(dst, size)], w1_sem.at[n])
        for n, (src, dst, size) in enumerate(spans)
    ]
    half_out = w2.shape[2]
    w2_copies = [
        pltpu.make_async_copy(
            w2_h.at[:, pl.ds(pl.multiple_of(side * half_out, LANES), half_out)], w2.at[n], w2_sem.at[n]
        )
        for n, side in enumerate((other, core))
    ]
    for copy in small[:4] + enc_copies:
        copy.wait()
    for copy in w1_copies + w2_copies:
        copy.start()

    lane = lax.broadcasted_iota(jnp.int32, route_src.shape, 1)
    route = jnp.full(route_src.shape, -1, jnp.int32)
    for s in range(samples):
        route = jnp.where(lane == s, seq_s[s] * samples + slot_s[s], route)
    route_src[...] = route
    routes[0] = route

    per = LANES // cap
    windows = lax.broadcasted_iota(jnp.int32, (BLOCK, LANES), 0)
    lanes_at = lax.broadcasted_iota(jnp.int32, (BLOCK, LANES), 1)

    def pool(s):
        pair, part = divmod(s, per)
        start = part * cap
        ids = jnp.concatenate([win_v[s : s + 1, :]] * per, axis=1)
        live = (lanes_at >= start) & (lanes_at < start + jnp.minimum(cnt_s[s], cap))
        hot = jnp.where((ids == windows) & live, 1.0, 0.0)
        number = jnp.sum(hot, axis=1, keepdims=True)
        total = lax.dot_general(
            hot.astype(jnp.bfloat16), enc[pair], (((1,), (1,)), ((), ())),
            preferred_element_type=jnp.float32,
        )
        y = (total * (1.0 / jnp.maximum(number, 1.0))).astype(jnp.bfloat16)
        for c in range(full):
            pooled[s, c * BLOCK : (c + 1) * BLOCK, :] = y[:, c * LANES : (c + 1) * LANES]
        if rem:
            tail = y[:, wide:]
            mid = BLOCK // 2
            pooled[s, full * BLOCK :, :] = jnp.concatenate([tail[:mid], tail[mid:]], axis=1)

    def pick(peer):
        chosen = jnp.int32(0)
        for s in range(1, samples):
            chosen = jnp.where(seq_s[s] == peer, jnp.int32(s), chosen)
        return pooled[chosen]

    half = groups // 2
    mine_base = me // half * half
    far_base = half - mine_base

    def far_first(i):
        far = lax.rem(me + i, half)
        near = lax.rem(me + i + 1, half)
        late = i // half
        peer = (1 - late) * (far_base + far) + late * (mine_base + near)
        return lax.rem(peer - me + groups, groups)

    def far_source(i):
        far = lax.rem(me - i + groups, half)
        near = lax.rem(me - i - 1 + 2 * groups, half)
        late = i // half
        peer = (1 - late) * (far_base + far) + late * (mine_base + near)
        return lax.rem(me - peer + groups, groups)

    def fill(j):
        outgo[j] = pick(lax.rem(me + j, groups))

    def data_copy(j):
        return pltpu.make_async_remote_copy(
            src_ref=outgo.at[j], dst_ref=arr.at[j], send_sem=send_sem.at[j], recv_sem=recv_sem.at[j],
            device_id={"dp": lax.rem(me + j, groups)}, device_id_type=MESH,
        )

    def route_copy(j):
        return pltpu.make_async_remote_copy(
            src_ref=route_src, dst_ref=routes.at[j], send_sem=rsend_sem.at[j], recv_sem=rrecv_sem.at[j],
            device_id={"dp": lax.rem(me + j, groups)}, device_id_type=MESH,
        )

    def forward(j):
        return pltpu.make_async_remote_copy(
            src_ref=arr.at[j], dst_ref=sib.at[j], send_sem=fsend_sem.at[j], recv_sem=frecv_sem.at[j],
            device_id={"tensor": other}, device_id_type=MESH,
        )

    for s in range(samples):
        pool(s)
    loop(2, lambda i: fill(far_first(i)))
    pl.semaphore_wait(barrier, groups)
    loop(groups - 1, lambda i: route_copy(i + 1).start())

    def stage(i):
        fill(far_first(i + 2))
        data_copy(far_first(i)).start()

    loop(groups - 3, stage)
    arr[0] = pick(me)
    data_copy(far_first(groups - 3)).start()
    data_copy(far_first(groups - 2)).start()
    forward(0).start()

    loop(groups - 1, lambda i: route_copy(i + 1).wait_recv())

    table = routes[...]
    source = lax.broadcasted_iota(jnp.int32, table.shape, 0)
    picks = [
        jnp.minimum(jnp.sum(jnp.where(table == me * samples + k, source, 0)), groups - 1)
        for k in range(samples)
    ]
    def arrive(i):
        j = far_source(i)
        data_copy(j).wait_recv()
        forward(j).start()

    loop(groups - 1, arrive)
    loop(groups, lambda i: forward(i).wait_recv())

    for k in range(samples):
        rows = slice(k * BLOCK, (k + 1) * BLOCK)
        for c in range(full):
            lanes = slice(c * LANES, (c + 1) * LANES)
            xbuf[rows, lanes] = arr[picks[k], c * BLOCK : (c + 1) * BLOCK, :]
            lanes = slice(wide + c * LANES, wide + (c + 1) * LANES)
            xbuf[rows, lanes] = sib[picks[k], c * BLOCK : (c + 1) * BLOCK, :]
        if rem:
            a = arr[picks[k], full * BLOCK :, :]
            b = sib[picks[k], full * BLOCK :, :]
            mid = BLOCK // 2
            lo = k * BLOCK
            xbuf[lo : lo + mid, 2 * wide :] = jnp.concatenate([a[:, :rem], b[:, :rem]], axis=1)
            xbuf[lo + mid : lo + 2 * mid, 2 * wide :] = jnp.concatenate([a[:, rem:], b[:, rem:]], axis=1)

    for copy in w1_copies + small[4:]:
        copy.wait()
    total_rows = samples * BLOCK
    step = min(256, total_rows)

    def first_layer(m):
        rows = pl.ds(m * step, step) if isinstance(m, int) else pl.ds(pl.multiple_of(m * step, step), step)
        for lo, size in col_chunks(w1.shape[1], 768):
            acc = jnp.dot(xbuf[rows, :], w1[:, lo : lo + size], preferred_element_type=jnp.float32)
            hidden[rows, lo : lo + size] = gelu(acc + b1_v[lo : lo + size]).astype(jnp.bfloat16)

    tiles = total_rows // step
    if tiles == 1:
        first_layer(0)
    else:
        pl.loop(0, tiles)(first_layer)
    for copy in w2_copies:
        copy.wait()

    chunks = col_chunks(half_out, 384)

    def part_copy(n):
        lo, size = chunks[n]
        return pltpu.make_async_remote_copy(
            src_ref=part_out.at[:, lo : lo + size], dst_ref=part_in.at[:, lo : lo + size],
            send_sem=psend_sem.at[n], recv_sem=precv_sem.at[n],
            device_id={"tensor": other}, device_id_type=MESH,
        )

    def over_rows(body):
        if tiles == 1:
            body(slice(0, step))
        else:

            @pl.loop(0, tiles)
            def _(m):
                body(pl.ds(pl.multiple_of(m * step, step), step))

    for n, (lo, size) in enumerate(chunks):

        def send_part(rows):
            part_out[rows, lo : lo + size] = jnp.dot(
                hidden[rows, :], w2[0, :, lo : lo + size], preferred_element_type=jnp.float32
            ).astype(jnp.bfloat16)

        over_rows(send_part)
        if n:
            part_copy(n - 1).start()
    for n, (lo, size) in enumerate(chunks):

        def keep_part(rows):
            out_v[rows, lo : lo + size] = jnp.dot(
                hidden[rows, :], w2[1, :, lo : lo + size], preferred_element_type=jnp.float32
            ).astype(jnp.bfloat16)

        over_rows(keep_part)
        if n == 0:
            part_copy(len(chunks) - 1).start()
    for n, (lo, size) in enumerate(chunks):
        part_copy(n).wait_recv()

        def finish(rows):
            lanes = slice(lo, lo + size)
            both = out_v[rows, lanes].astype(jnp.float32) + part_in[rows, lanes].astype(jnp.float32)
            out_v[rows, lanes] = (both + b2_v[lanes]).astype(jnp.bfloat16)

        over_rows(finish)
    loop(groups, lambda i: forward(i).wait_send())

    def drain(i):
        data_copy(i + 1).wait_send()
        route_copy(i + 1).wait_send()

    loop(groups - 1, drain)
    for n in range(len(chunks)):
        part_copy(n).wait_send()


def shards(encoded, counts, win_ids, dest_seq, dest_slot, w_first, b_first, w_second, b_second):
    samples, cap = win_ids.shape
    feat = encoded.shape[1]
    groups = lax.axis_size("dp")
    hid = w_first.shape[1]
    half_out = b_second.shape[0]
    rows = samples * BLOCK
    block_rows = BLOCK * feat // LANES
    chunks = len(col_chunks(half_out, 384))
    vmem = pl.BlockSpec(memory_space=pltpu.VMEM)
    hbm = pl.BlockSpec(memory_space=pltpu.HBM)
    bf16 = jnp.bfloat16
    dma = pltpu.SemaphoreType.DMA
    return pl.pallas_call(
        functools.partial(kernel, (groups, samples, cap, feat)),
        out_shape=pltpu.VMEM((rows, half_out), bf16),
        in_specs=[hbm] * 9,
        out_specs=vmem,
        scratch_shapes=[
            pltpu.SMEM((samples,), jnp.int32), pltpu.SMEM((samples,), jnp.int32), pltpu.SMEM((samples,), jnp.int32),
            pltpu.VMEM((samples, cap), jnp.int32), pltpu.VMEM((hid,), jnp.float32), pltpu.VMEM((half_out,), jnp.float32),
            pltpu.VMEM((samples * cap // LANES, feat, LANES), bf16),
            pltpu.VMEM((2 * feat, hid), bf16),
            pltpu.VMEM((2, hid, half_out), bf16),
            pltpu.VMEM((samples, block_rows, LANES), bf16),
            pltpu.VMEM((groups, block_rows, LANES), bf16),
            pltpu.VMEM((groups, block_rows, LANES), bf16),
            pltpu.VMEM((groups, block_rows, LANES), bf16),
            pltpu.VMEM((1, LANES), jnp.int32),
            pltpu.VMEM((groups, 1, LANES), jnp.int32),
            pltpu.VMEM((rows, 2 * feat), bf16),
            pltpu.VMEM((rows, hid), bf16),
            pltpu.VMEM((rows, half_out), bf16),
            pltpu.VMEM((rows, half_out), bf16),
            dma((6,)), dma((samples * cap // LANES,)), dma((4,)), dma((2,)),
            dma((groups,)), dma((groups,)), dma((groups,)), dma((groups,)), dma((groups,)), dma((groups,)),
            dma((chunks,)), dma((chunks,)),
        ],
        compiler_params=pltpu.CompilerParams(
            collective_id=0, has_side_effects=True, vmem_limit_bytes=60 * 1024 * 1024
        ),
    )(
        dest_seq, dest_slot, counts, win_ids, b_first, b_second, encoded.T, w_first, w_second,
    )


def solution(mesh):
    placed = (
        P("dp", "tensor"), P("dp"), P("dp", None), P("dp"), P("dp"),
        P(None, "tensor"), P("tensor"), P("tensor", None), P("tensor"),
    )
    return jax.shard_map(
        shards, mesh=mesh, in_specs=placed, out_specs=P("dp", "tensor"), check_vma=False
    )
```

```python
import functools
import math

import jax
import jax.numpy as jnp
from jax import lax
from jax.experimental import pallas as pl
from jax.experimental.pallas import tpu as pltpu
from jax.sharding import PartitionSpec as P

BLOCK = 32
LANES = 128
WIDE = 512
MESH = pl.DeviceIdType.MESH
UNROLL_MAX = 16
scope = jax.named_scope


def loop(count, body):
    if count <= UNROLL_MAX:
        for i in range(count):
            body(i)
    else:

        @pl.loop(0, count)
        def _(i):
            body(i)


def col_chunks(lo, hi, step):
    return [(at, min(step, hi - at)) for at in range(lo, hi, step)]


def gelu(x):
    c0 = math.sqrt(2.0 / math.pi)
    half = 0.5 * x
    return half + half * jnp.tanh(x * (c0 + (c0 * 0.044715) * (x * x)))


def exchange_masks(groups):
    quarter, half = groups // 4, groups // 2
    bits = quarter.bit_length() - 1
    plane = [int(format(g, f"0{bits}b")[::-1], 2) if bits else 0 for g in range(quarter)]
    near = [m for m in plane] + [quarter + m for m in plane]
    far = [half + z * quarter + m for m in plane for z in (1, 0)]
    return near + far


def flip(me, mask, groups):
    total, bit = 0, 1
    while bit < groups:
        own = lax.rem(me // bit, 2)
        total = total + bit * ((1 - own) if mask & bit else own)
        bit *= 2
    return total


def kernel(
    dims,
    seq_h, slot_h, cnt_h, win_h, b1_h, b2_h, enc_h, w1_h, w2_h,
    out_v,
    seq_s, slot_s, cnt_s, win_v, b1_v, b2_v, val_s, pick_s, rank_s,
    enc, w1, w2, pooled, outgo, arr_a, arr_b, sib_a, sib_b, route_src, routes,
    x_mine, x_sib, pre, hidden, keep, *rest,
):
    groups, samples, cap, feat, parts = dims
    part_out, part_in = rest[:parts], rest[parts : 2 * parts]
    (small_sem, load_sem, w1_sem, w2_sem, send_sem, recv_sem, rsend_sem, rrecv_sem, fsend_sem, frecv_sem,
     psend_sem, precv_sem) = rest[2 * parts :]
    full = feat // LANES
    rem = feat - full * LANES
    wide = full * LANES
    hid = w1.shape[2]
    half_out = b2_v.shape[0]
    first = arr_a.shape[0]
    ranks = samples // 2
    tile = ranks * BLOCK
    me = lax.axis_index("dp")
    core = lax.axis_index("tensor")
    other = 1 - core
    masks = exchange_masks(groups)
    peers = [flip(me, mask, groups) for mask in masks]
    order = list(range(1, groups))

    barrier = pltpu.get_barrier_semaphore()
    for o in range(1, groups):
        pl.semaphore_signal(barrier, 1, device_id={"dp": peers[o]}, device_id_type=MESH)
    pl.semaphore_signal(barrier, 1, device_id={"tensor": other}, device_id_type=MESH)

    pairs = enc.shape[0]
    enc_copies = [
        pltpu.make_async_copy(enc_h.at[:, p * LANES : (p + 1) * LANES], enc.at[p], load_sem.at[p])
        for p in range(pairs)
    ]
    small = [
        pltpu.make_async_copy(src, dst, small_sem.at[n])
        for n, (src, dst) in enumerate(
            [(seq_h, seq_s), (slot_h, slot_s), (cnt_h, cnt_s), (win_h, win_v), (b1_h, b1_v), (b2_h, b2_v)]
        )
    ]
    for copy in small[:4] + enc_copies + small[4:]:
        copy.start()
    w1_copies = [
        pltpu.make_async_copy(w1_h.at[pl.ds(pl.multiple_of(side * feat, 64), feat)], w1.at[n], w1_sem.at[n])
        for n, side in enumerate((core, other))
    ]
    w2_copies = [
        pltpu.make_async_copy(
            w2_h.at[:, pl.ds(pl.multiple_of(side * half_out, LANES), half_out)],
            w2.at[:, n * half_out : (n + 1) * half_out], w2_sem.at[n],
        )
        for n, side in enumerate((other, core))
    ]
    with scope("loadwait"):
        for copy in small[:4] + enc_copies:
            copy.wait()
    for copy in w1_copies + w2_copies:
        copy.start()

    lane = lax.broadcasted_iota(jnp.int32, route_src.shape, 1)
    route = jnp.full(route_src.shape, -1, jnp.int32)
    for s in range(samples):
        route = jnp.where(lane == s, seq_s[s] * samples + slot_s[s], route)
    route_src[...] = route
    routes[0] = route

    per = LANES // cap
    windows = lax.broadcasted_iota(jnp.int32, (BLOCK, LANES), 0)
    lanes_at = lax.broadcasted_iota(jnp.int32, (BLOCK, LANES), 1)

    def pool(s):
        pair, part = divmod(s, per)
        start = part * cap
        ids = jnp.concatenate([win_v[s : s + 1, :]] * per, axis=1)
        live = (lanes_at >= start) & (lanes_at < start + jnp.minimum(cnt_s[s], cap))
        hot = jnp.where((ids == windows) & live, 1.0, 0.0)
        number = jnp.sum(hot, axis=1, keepdims=True)
        total = lax.dot_general(
            hot.astype(jnp.bfloat16), enc[pair], (((1,), (1,)), ((), ())),
            preferred_element_type=jnp.float32,
        )
        y = (total * (1.0 / jnp.maximum(number, 1.0))).astype(jnp.bfloat16)
        for c in range(full):
            pooled[s, c * BLOCK : (c + 1) * BLOCK, :] = y[:, c * LANES : (c + 1) * LANES]
        if rem:
            tail = y[:, wide:]
            mid = BLOCK // 2
            pooled[s, full * BLOCK :, :] = jnp.concatenate([tail[:mid], tail[mid:]], axis=1)

    def pick(peer):
        chosen = jnp.int32(0)
        for s in range(1, samples):
            chosen = jnp.where(seq_s[s] == peer, jnp.int32(s), chosen)
        return pooled[chosen]

    def place(o, near_ref, late_ref):
        return near_ref.at[o] if o < first else late_ref.at[o - first]

    def data_copy(o):
        return pltpu.make_async_remote_copy(
            src_ref=outgo.at[o], dst_ref=place(o, arr_a, arr_b), send_sem=send_sem.at[o], recv_sem=recv_sem.at[o],
            device_id={"dp": peers[o]}, device_id_type=MESH,
        )

    def route_copy(o):
        return pltpu.make_async_remote_copy(
            src_ref=route_src, dst_ref=routes.at[o], send_sem=rsend_sem.at[o], recv_sem=rrecv_sem.at[o],
            device_id={"dp": peers[o]}, device_id_type=MESH,
        )

    def forward(o):
        return pltpu.make_async_remote_copy(
            src_ref=place(o, arr_a, arr_b), dst_ref=place(o, sib_a, sib_b),
            send_sem=fsend_sem.at[o], recv_sem=frecv_sem.at[o],
            device_id={"tensor": other}, device_id_type=MESH,
        )

    with scope("pool"):
        for s in range(samples):
            pool(s)

    def fill(o):
        outgo[o] = pick(peers[o])

    ahead = 2
    for o in order[:ahead]:
        fill(o)
    with scope("barrier"):
        pl.semaphore_wait(barrier, groups)
    with scope("stage"):
        for o in order:
            route_copy(o).start()
        for n, o in enumerate(order):
            if n + ahead < len(order):
                fill(order[n + ahead])
            else:
                arr_a[0] = pick(me)
            data_copy(o).start()
        forward(0).start()

    with scope("routewait"):
        for o in order:
            route_copy(o).wait_recv()
    base = me * samples
    seen = jnp.int32(0)
    for o in range(groups):
        row = routes[o]
        hit = (row >= base) & (row < base + samples)
        value = jnp.sum(jnp.where(hit, row - base + 1, 0))
        val_s[o] = value
        val_s[groups + o] = seen
        seen = seen + jnp.minimum(value, 1)

    def find(r):
        at, spot = jnp.int32(0), jnp.int32(0)
        for o in range(groups):
            value, before = val_s[o], val_s[groups + o]
            at = jnp.where((value > 0) & (before == r), o, at)
            spot = jnp.where(value == r + 1, before, spot)
        pick_s[r] = at
        rank_s[r] = jnp.minimum(spot, samples - 1)

    with scope("picks"):
        loop(samples, find)

    def arrive(o):
        with scope(f"arr{o}"):
            data_copy(o).wait_recv()
        forward(o).start()

    def unpack(dst, r, block):
        lo = r * BLOCK if isinstance(r, int) else pl.multiple_of(r * BLOCK, BLOCK)
        for c in range(full):
            dst[pl.ds(lo, BLOCK), c * LANES : (c + 1) * LANES] = block[c * BLOCK : (c + 1) * BLOCK]
        if rem:
            mid = BLOCK // 2
            tail = block[full * BLOCK :]
            dst[pl.ds(lo, mid), wide:] = tail[:, :rem]
            dst[pl.ds(lo + mid, mid), wide:] = tail[:, rem:]

    def early(dst, ref):
        def one(r):
            unpack(dst, r, ref[jnp.minimum(pick_s[r], first - 1)])

        loop(ranks, one)

    def late(dst, ref, ref_late):
        def one(r):
            at = pick_s[ranks + r]
            a = ref[jnp.minimum(at, first - 1)]
            b = ref_late[jnp.maximum(at - first, 0)]
            unpack(dst, r, jnp.where(at < first, a, b))

        loop(ranks, one)

    step = min(256, tile)

    def over_rows(body):
        if tile == step:
            body(slice(0, step), 0)
        else:

            @pl.loop(0, tile // step)
            def _(m):
                body(pl.ds(pl.multiple_of(m * step, step), step), m * (step // BLOCK))

    up_chunks = col_chunks(0, hid, 768)

    def mine_part(rows, _):
        for lo, size in up_chunks:
            pre[rows, lo : lo + size] = jnp.dot(
                x_mine[rows, :], w1[0, :, lo : lo + size], preferred_element_type=jnp.float32
            )

    def sib_part(rows, _):
        for lo, size in up_chunks:
            acc = jnp.dot(x_sib[rows, :], w1[1, :, lo : lo + size], preferred_element_type=jnp.float32)
            acc = acc + pre[rows, lo : lo + size] + b1_v[lo : lo + size]
            hidden[rows, lo : lo + size] = gelu(acc).astype(jnp.bfloat16)

    outs = col_chunks(0, half_out, WIDE)
    even = half_out // 256 * 256
    spans = col_chunks(0, even, WIDE)
    if even < half_out:
        spans = spans + [(even, 256)]
    spans = spans + col_chunks(sum(spans[-1]), 2 * half_out, WIDE)

    def down(which, lo, size):
        def body(rows, at):
            y = jnp.dot(
                hidden[rows, :], w2[:, lo : lo + size], preferred_element_type=jnp.float32
            ).astype(jnp.bfloat16)
            for n, (start, width) in enumerate(outs):
                begin, end = max(lo, start), min(lo + size, start + width)
                if begin < end:
                    for r in range(step // BLOCK):
                        part_out[n][which * ranks + at + r, :, begin - start : end - start] = y[
                            r * BLOCK : (r + 1) * BLOCK, begin - lo : end - lo
                        ]
            begin = max(lo, half_out)
            if begin < lo + size:
                for r in range(step // BLOCK):
                    keep[which * ranks + at + r, :, begin - half_out : lo + size - half_out] = y[
                        r * BLOCK : (r + 1) * BLOCK, begin - lo :
                    ]

        over_rows(body)

    def part_copy(which, n):
        span = pl.ds(which * ranks, ranks)
        return pltpu.make_async_remote_copy(
            src_ref=part_out[n].at[span], dst_ref=part_in[n].at[span],
            send_sem=psend_sem.at[which * parts + n], recv_sem=precv_sem.at[which * parts + n],
            device_id={"tensor": other}, device_id_type=MESH,
        )

    def project(which, between):
        sent = 0
        for at, (lo, size) in enumerate(spans):
            with scope(f"down{which}_{at}"):
                down(which, lo, size)
            while sent < parts and sum(outs[sent]) <= spans[at - 1][0] + spans[at - 1][1] and at:
                part_copy(which, sent).start()
                sent += 1
            between(at)

    for o in range(1, first):
        arrive(o)
    with scope("fwdA"):
        for o in range(first):
            forward(o).wait_recv()
    with scope("xA"):
        early(x_mine, arr_a)
        early(x_sib, sib_a)
    with scope("w1wait"):
        for copy in w1_copies + small[4:]:
            copy.wait()
    with scope("upA"):
        over_rows(mine_part)
        over_rows(sib_part)
    pending = list(range(first, groups))
    share = max(1, len(pending) // 4)

    def take(_):
        for o in pending[:share]:
            arrive(o)
        del pending[:share]

    take(0)
    with scope("w2wait"):
        for copy in w2_copies:
            copy.wait()
    project(0, lambda at: take(0) if at in (2, len(spans) - 1) else None)
    while pending:
        take(0)
    with scope("xBm"):
        late(x_mine, arr_a, arr_b)
    with scope("upBm"):
        over_rows(mine_part)
    with scope("fwdB"):
        for o in range(first, groups):
            forward(o).wait_recv()
    with scope("xBs"):
        late(x_sib, sib_a, sib_b)
    with scope("upBs"):
        over_rows(sib_part)
    project(1, lambda at: None)
    for n, (lo, size) in enumerate(outs):
        with scope(f"pwait{n}"):
            part_copy(0, n).wait_recv()
            part_copy(1, n).wait_recv()

        def finish(k):
            r = rank_s[k]
            rows = pl.ds(k * BLOCK if isinstance(k, int) else pl.multiple_of(k * BLOCK, BLOCK), BLOCK)
            both = keep[r, :, lo : lo + size].astype(jnp.float32) + part_in[n][r].astype(jnp.float32)
            out_v[rows, lo : lo + size] = (both + b2_v[lo : lo + size]).astype(jnp.bfloat16)

        with scope(f"finish{n}"):
            loop(samples, finish)
    with scope("drain"):
        for o in range(groups):
            forward(o).wait_send()
        for o in order:
            data_copy(o).wait_send()
            route_copy(o).wait_send()
        for which in range(2):
            for n in range(parts):
                part_copy(which, n).wait_send()


def shards(encoded, counts, win_ids, dest_seq, dest_slot, w_first, b_first, w_second, b_second):
    samples, cap = win_ids.shape
    feat = encoded.shape[1]
    groups = lax.axis_size("dp")
    hid = w_first.shape[1]
    half_out = b_second.shape[0]
    rows = samples * BLOCK
    tile = rows // 2
    block_rows = BLOCK * feat // LANES
    outs = col_chunks(0, half_out, WIDE)
    parts = len(outs)
    late = samples // 2
    first = groups - late
    hbm = pl.BlockSpec(memory_space=pltpu.HBM)
    bf16, f32, i32 = jnp.bfloat16, jnp.float32, jnp.int32
    vmem, smem, dma = pltpu.VMEM, pltpu.SMEM, pltpu.SemaphoreType.DMA
    return pl.pallas_call(
        functools.partial(kernel, (groups, samples, cap, feat, parts)),
        out_shape=vmem((rows, half_out), bf16),
        in_specs=[hbm] * 9,
        out_specs=pl.BlockSpec(memory_space=pltpu.VMEM),
        scratch_shapes=[
            smem((samples,), i32), smem((samples,), i32), smem((samples,), i32),
            vmem((samples, cap), i32), vmem((hid,), f32), vmem((half_out,), f32),
            smem((2 * groups,), i32), smem((samples,), i32), smem((samples,), i32),
            vmem((samples * cap // LANES, feat, LANES), bf16),
            vmem((2, feat, hid), bf16),
            vmem((hid, 2 * half_out), bf16),
            vmem((samples, block_rows, LANES), bf16),
            vmem((groups, block_rows, LANES), bf16),
            vmem((first, block_rows, LANES), bf16),
            vmem((late, block_rows, LANES), bf16),
            vmem((first, block_rows, LANES), bf16),
            vmem((late, block_rows, LANES), bf16),
            vmem((1, LANES), i32),
            vmem((groups, 1, LANES), i32),
            vmem((tile, feat), bf16),
            vmem((tile, feat), bf16),
            vmem((tile, hid), f32),
            vmem((tile, hid), bf16),
            vmem((samples, BLOCK, half_out), bf16),
            *[vmem((samples, BLOCK, size), bf16) for _, size in outs],
            *[vmem((samples, BLOCK, size), bf16) for _, size in outs],
            dma((6,)), dma((samples * cap // LANES,)), dma((2,)), dma((2,)),
            dma((groups,)), dma((groups,)), dma((groups,)), dma((groups,)), dma((groups,)), dma((groups,)),
            dma((2 * parts,)), dma((2 * parts,)),
        ],
        compiler_params=pltpu.CompilerParams(
            collective_id=0, has_side_effects=True, vmem_limit_bytes=60 * 1024 * 1024
        ),
    )(
        dest_seq, dest_slot, counts, win_ids, b_first, b_second, encoded.T, w_first, w_second,
    )


def solution(mesh):
    placed = (
        P("dp", "tensor"), P("dp"), P("dp", None), P("dp"), P("dp"),
        P(None, "tensor"), P("tensor"), P("tensor", None), P("tensor"),
    )
    return jax.shard_map(
        shards, mesh=mesh, in_specs=placed, out_specs=P("dp", "tensor"), check_vma=False
    )
```

```python
import functools
import math

import jax
import jax.numpy as jnp
from jax import lax
from jax.experimental import pallas as pl
from jax.experimental.pallas import tpu as pltpu
from jax.sharding import PartitionSpec as P

BLOCK = 32
LANES = 128
WIDE = 512
MESH = pl.DeviceIdType.MESH
UNROLL_MAX = 16
scope = jax.named_scope


def loop(count, body):
    if count <= UNROLL_MAX:
        for i in range(count):
            body(i)
    else:

        @pl.loop(0, count)
        def _(i):
            body(i)


def col_chunks(lo, hi, step):
    return [(at, min(step, hi - at)) for at in range(lo, hi, step)]


def gelu(x):
    c0 = math.sqrt(2.0 / math.pi)
    half = 0.5 * x
    return half + half * jnp.tanh(x * (c0 + (c0 * 0.044715) * (x * x)))


def settle(ref, sem):
    pltpu.make_async_copy(ref, ref, sem).wait()


def exchange_masks(groups):
    quarter, half = groups // 4, groups // 2
    bits = quarter.bit_length() - 1
    plane = [int(format(g, f"0{bits}b")[::-1], 2) if bits else 0 for g in range(quarter)]
    near = [m for m in plane] + [quarter + m for m in plane]
    far = [half + z * quarter + m for m in plane for z in (1, 0)]
    return near + far


def flip(me, mask, groups):
    total, bit = 0, 1
    while bit < groups:
        own = lax.rem(me // bit, 2)
        total = total + bit * ((1 - own) if mask & bit else own)
        bit *= 2
    return total


def kernel(
    dims,
    seq_h, slot_h, cnt_h, win_h, b1_h, b2_h, enc_h, w1_h, w2_h,
    out_v,
    seq_s, slot_s, cnt_s, win_v, b1_v, b2_v, val_s, pick_s, rank_s,
    enc, w1, w2, pooled, outgo, arr_a, arr_b, sib_a, sib_b, route_src, routes,
    x_mine, x_sib, pre, hidden, keep, *rest,
):
    groups, samples, cap, feat, parts = dims
    part_out, part_in = rest[:parts], rest[parts : 2 * parts]
    small_sem, load_sem, send_sem, recv_sem, group_sem, psend_sem, precv_sem = rest[2 * parts :]
    full = feat // LANES
    rem = feat - full * LANES
    wide = full * LANES
    hid = w1.shape[2]
    half_out = b2_v.shape[0]
    first = arr_a.shape[0]
    ranks = samples // 2
    tile = ranks * BLOCK
    me = lax.axis_index("dp")
    core = lax.axis_index("tensor")
    other = 1 - core
    masks = exchange_masks(groups)
    peers = [flip(me, mask, groups) for mask in masks]
    order = list(range(1, groups))
    half = groups // 2
    depth = me // (groups // 4)
    inner = lax.rem((depth + 1) // 2, 2)

    barrier = pltpu.get_barrier_semaphore()
    for o in range(1, groups):
        pl.semaphore_signal(barrier, 1, device_id={"dp": peers[o]}, device_id_type=MESH)
    pl.semaphore_signal(barrier, 1, device_id={"tensor": other}, device_id_type=MESH)

    pairs = enc.shape[0]
    enc_copies = [
        pltpu.make_async_copy(enc_h.at[:, p * LANES : (p + 1) * LANES], enc.at[p], load_sem.at[0])
        for p in range(pairs)
    ]
    small = [
        pltpu.make_async_copy(src, dst, small_sem.at[n])
        for n, (src, dst) in enumerate(
            [(seq_h, seq_s), (slot_h, slot_s), (cnt_h, cnt_s), (win_h, win_v), (b1_h, b1_v), (b2_h, b2_v)]
        )
    ]
    for copy in small[:4] + enc_copies + small[4:]:
        copy.start()
    w1_copies = [
        pltpu.make_async_copy(w1_h.at[pl.ds(pl.multiple_of(side * feat, 64), feat)], w1.at[n], load_sem.at[1])
        for n, side in enumerate((core, other))
    ]
    w2_copies = [
        pltpu.make_async_copy(
            w2_h.at[:, pl.ds(pl.multiple_of(side * half_out, LANES), half_out)],
            w2.at[:, n * half_out : (n + 1) * half_out], load_sem.at[2],
        )
        for n, side in enumerate((other, core))
    ]
    with scope("loadwait"):
        for copy in small[:4]:
            copy.wait()
        settle(enc, load_sem.at[0])
    for copy in w1_copies + w2_copies:
        copy.start()

    lane = lax.broadcasted_iota(jnp.int32, route_src.shape, 1)
    route = jnp.full(route_src.shape, -1, jnp.int32)
    for s in range(samples):
        route = jnp.where(lane == s, seq_s[s] * samples + slot_s[s], route)
    route_src[...] = route
    routes[0] = route

    per = LANES // cap
    tall = per * BLOCK
    row_at = lax.broadcasted_iota(jnp.int32, (tall, LANES), 0)
    lane_at = lax.broadcasted_iota(jnp.int32, (tall, LANES), 1)
    windows = lax.rem(row_at, BLOCK)
    slot_at = lane_at - row_at // BLOCK * cap

    def pool(pair):
        at = pair * per
        ids = jnp.concatenate([win_v[at + n : at + n + 1, :] for n in range(per)], axis=1)
        limit = jnp.full((tall, LANES), jnp.minimum(cnt_s[at], cap))
        for n in range(1, per):
            limit = jnp.where(row_at >= n * BLOCK, jnp.minimum(cnt_s[at + n], cap), limit)
        live = (slot_at >= 0) & (slot_at < limit)
        hot = jnp.where((ids == windows) & live, 1.0, 0.0)
        number = jnp.sum(hot, axis=1, keepdims=True)
        total = lax.dot_general(
            hot.astype(jnp.bfloat16), enc[pair], (((1,), (1,)), ((), ())),
            preferred_element_type=jnp.float32,
        )
        y = (total * (1.0 / jnp.maximum(number, 1.0))).astype(jnp.bfloat16)
        for n in range(per):
            rows = y[n * BLOCK : (n + 1) * BLOCK]
            for c in range(full):
                pooled[at + n, c * BLOCK : (c + 1) * BLOCK, :] = rows[:, c * LANES : (c + 1) * LANES]
            if rem:
                tail = rows[:, wide:]
                mid = BLOCK // 2
                pooled[at + n, full * BLOCK :, :] = jnp.concatenate([tail[:mid], tail[mid:]], axis=1)

    def pick(peer):
        chosen = jnp.int32(0)
        for s in range(1, samples):
            chosen = jnp.where(seq_s[s] == peer, jnp.int32(s), chosen)
        return pooled[chosen]

    def place(o, near_ref, late_ref):
        return near_ref.at[o] if o < first else late_ref.at[o - first]

    def swapped(o):
        if o < half:
            return o, peers[o]
        low = o - (o - half) % 2
        lead = inner if o == low else 1 - inner
        return low + lead, lead * peers[low + 1] + (1 - lead) * peers[low]

    def send(o):
        slot, peer = swapped(o)
        home, at = (arr_a, slot) if o < first else (arr_b, slot - first)
        return pltpu.make_async_remote_copy(
            src_ref=outgo.at[slot], dst_ref=home.at[at], send_sem=send_sem.at[0], recv_sem=recv_sem.at[slot],
            device_id={"dp": peer}, device_id_type=MESH,
        )

    def data_copy(o):
        return pltpu.make_async_remote_copy(
            src_ref=outgo.at[o], dst_ref=place(o, arr_a, arr_b), send_sem=send_sem.at[0], recv_sem=recv_sem.at[o],
            device_id={"dp": peers[o]}, device_id_type=MESH,
        )

    def route_copy(o):
        return pltpu.make_async_remote_copy(
            src_ref=route_src, dst_ref=routes.at[o], send_sem=send_sem.at[1], recv_sem=group_sem.at[0],
            device_id={"dp": peers[o]}, device_id_type=MESH,
        )

    def forward(o):
        late_slot = int(o >= first)
        return pltpu.make_async_remote_copy(
            src_ref=place(o, arr_a, arr_b), dst_ref=place(o, sib_a, sib_b),
            send_sem=send_sem.at[2 + late_slot], recv_sem=group_sem.at[1 + late_slot],
            device_id={"tensor": other}, device_id_type=MESH,
        )

    with scope("pool"):
        for pair in range(pairs):
            pool(pair)

    def fill(o):
        slot, peer = swapped(o)
        outgo[slot] = pick(peer)

    ahead = 2
    for o in order[:ahead]:
        fill(o)
    with scope("barrier"):
        pl.semaphore_wait(barrier, groups)
    with scope("stage"):
        for o in order:
            route_copy(o).start()
        for n, o in enumerate(order[: first - 1]):
            fill(order[n + ahead])
            send(o).start()
        for o in order[first - 1 + ahead :]:
            fill(o)
        arr_a[0] = pick(me)

        @pl.when(core == 0)
        def _():
            for o in order[first - 1 :]:
                send(o).start()

        forward(0).start()

    with scope("routewait"):
        settle(routes.at[1:], group_sem.at[0])
    base = me * samples
    seen = jnp.int32(0)
    for o in range(groups):
        row = routes[o]
        hit = (row >= base) & (row < base + samples)
        value = jnp.sum(jnp.where(hit, row - base + 1, 0))
        val_s[o] = value
        val_s[groups + o] = seen
        seen = seen + jnp.minimum(value, 1)

    def find(r):
        at, spot = jnp.int32(0), jnp.int32(0)
        for o in range(groups):
            value, before = val_s[o], val_s[groups + o]
            at = jnp.where((value > 0) & (before == r), o, at)
            spot = jnp.where(value == r + 1, before, spot)
        pick_s[r] = at
        rank_s[r] = jnp.minimum(spot, samples - 1)

    with scope("picks"):
        loop(samples, find)

    def arrive(o):
        with scope(f"arr{o}"):
            data_copy(o).wait_recv()
        forward(o).start()

    def unpack(dst, r, block):
        lo = r * BLOCK if isinstance(r, int) else pl.multiple_of(r * BLOCK, BLOCK)
        for c in range(full):
            dst[pl.ds(lo, BLOCK), c * LANES : (c + 1) * LANES] = block[c * BLOCK : (c + 1) * BLOCK]
        if rem:
            mid = BLOCK // 2
            tail = block[full * BLOCK :]
            dst[pl.ds(lo, mid), wide:] = tail[:, :rem]
            dst[pl.ds(lo + mid, mid), wide:] = tail[:, rem:]

    def early(dst, ref):
        def one(r):
            unpack(dst, r, ref[jnp.minimum(pick_s[r], first - 1)])

        loop(ranks, one)

    def late(dst, ref, ref_late):
        def one(r):
            at = pick_s[ranks + r]
            a = ref[jnp.minimum(at, first - 1)]
            b = ref_late[jnp.maximum(at - first, 0)]
            unpack(dst, r, jnp.where(at < first, a, b))

        loop(ranks, one)

    step = min(256, tile)

    def over_rows(body):
        if tile == step:
            body(slice(0, step), 0)
        else:

            @pl.loop(0, tile // step)
            def _(m):
                body(pl.ds(pl.multiple_of(m * step, step), step), m * (step // BLOCK))

    up_chunks = col_chunks(0, hid, 768)

    def mine_part(rows, _):
        for lo, size in up_chunks:
            pre[rows, lo : lo + size] = jnp.dot(
                x_mine[rows, :], w1[0, :, lo : lo + size], preferred_element_type=jnp.float32
            )

    def sib_part(rows, _):
        for lo, size in up_chunks:
            acc = jnp.dot(x_sib[rows, :], w1[1, :, lo : lo + size], preferred_element_type=jnp.float32)
            acc = acc + pre[rows, lo : lo + size] + b1_v[lo : lo + size]
            hidden[rows, lo : lo + size] = gelu(acc).astype(jnp.bfloat16)

    outs = col_chunks(0, half_out, WIDE)
    even = half_out // 256 * 256
    spans = col_chunks(0, even, WIDE)
    if even < half_out:
        spans = spans + [(even, 256)]
    spans = spans + col_chunks(sum(spans[-1]), 2 * half_out, WIDE)

    def down(which, lo, size):
        def body(rows, at):
            y = jnp.dot(
                hidden[rows, :], w2[:, lo : lo + size], preferred_element_type=jnp.float32
            ).astype(jnp.bfloat16)
            for n, (start, width) in enumerate(outs):
                begin, end = max(lo, start), min(lo + size, start + width)
                if begin < end:
                    for r in range(step // BLOCK):
                        part_out[n][which * ranks + at + r, :, begin - start : end - start] = y[
                            r * BLOCK : (r + 1) * BLOCK, begin - lo : end - lo
                        ]
            begin = max(lo, half_out)
            if begin < lo + size:
                for r in range(step // BLOCK):
                    keep[which * ranks + at + r, :, begin - half_out : lo + size - half_out] = y[
                        r * BLOCK : (r + 1) * BLOCK, begin - lo :
                    ]

        over_rows(body)

    def part_copy(which, n):
        span = pl.ds(which * ranks, ranks)
        return pltpu.make_async_remote_copy(
            src_ref=part_out[n].at[span], dst_ref=part_in[n].at[span],
            send_sem=psend_sem.at[n], recv_sem=precv_sem.at[n],
            device_id={"tensor": other}, device_id_type=MESH,
        )

    def project(which):
        with scope(f"send{which}"):
            for lo, size in spans:
                if lo < half_out:
                    down(which, lo, size)
        for n in range(parts):
            part_copy(which, n).start()
        with scope(f"keep{which}"):
            for lo, size in spans:
                if lo >= half_out:
                    down(which, lo, size)

    for o in range(1, first):
        arrive(o)

    @pl.when(core == 1)
    def _():
        for o in order[first - 1 :]:
            send(o).start()

    with scope("fwdA"):
        settle(sib_a, group_sem.at[1])
    with scope("xA"):
        early(x_mine, arr_a)
        early(x_sib, sib_a)
    with scope("w1wait"):
        settle(w1, load_sem.at[1])
        for copy in small[4:]:
            copy.wait()
    with scope("upA"):
        over_rows(mine_part)
        over_rows(sib_part)
    with scope("w2wait"):
        settle(w2, load_sem.at[2])
    project(0)
    for o in range(first, groups):
        arrive(o)
    with scope("xBm"):
        late(x_mine, arr_a, arr_b)
    with scope("upBm"):
        over_rows(mine_part)
    with scope("fwdB"):
        settle(sib_b, group_sem.at[2])
    with scope("xBs"):
        late(x_sib, sib_a, sib_b)
    with scope("upBs"):
        over_rows(sib_part)
    project(1)
    for n, (lo, size) in enumerate(outs):
        with scope(f"pwait{n}"):
            settle(part_in[n], precv_sem.at[n])

        def finish(k):
            r = rank_s[k]
            rows = pl.ds(k * BLOCK if isinstance(k, int) else pl.multiple_of(k * BLOCK, BLOCK), BLOCK)
            both = keep[r, :, lo : lo + size].astype(jnp.float32) + part_in[n][r].astype(jnp.float32)
            out_v[rows, lo : lo + size] = (both + b2_v[lo : lo + size]).astype(jnp.bfloat16)

        with scope(f"finish{n}"):
            loop(samples, finish)
    with scope("drain"):
        settle(arr_a, send_sem.at[2])
        settle(arr_b, send_sem.at[3])
        settle(outgo.at[1:], send_sem.at[0])
        settle(routes.at[1:], send_sem.at[1])
        for n in range(parts):
            settle(part_out[n], psend_sem.at[n])


def shards(encoded, counts, win_ids, dest_seq, dest_slot, w_first, b_first, w_second, b_second):
    samples, cap = win_ids.shape
    feat = encoded.shape[1]
    groups = lax.axis_size("dp")
    hid = w_first.shape[1]
    half_out = b_second.shape[0]
    rows = samples * BLOCK
    tile = rows // 2
    block_rows = BLOCK * feat // LANES
    outs = col_chunks(0, half_out, WIDE)
    parts = len(outs)
    late = samples // 2
    first = groups - late
    hbm = pl.BlockSpec(memory_space=pltpu.HBM)
    bf16, f32, i32 = jnp.bfloat16, jnp.float32, jnp.int32
    vmem, smem, dma = pltpu.VMEM, pltpu.SMEM, pltpu.SemaphoreType.DMA
    return pl.pallas_call(
        functools.partial(kernel, (groups, samples, cap, feat, parts)),
        out_shape=vmem((rows, half_out), bf16),
        in_specs=[hbm] * 9,
        out_specs=pl.BlockSpec(memory_space=pltpu.VMEM),
        scratch_shapes=[
            smem((samples,), i32), smem((samples,), i32), smem((samples,), i32),
            vmem((samples, cap), i32), vmem((hid,), f32), vmem((half_out,), f32),
            smem((2 * groups,), i32), smem((samples,), i32), smem((samples,), i32),
            vmem((samples * cap // LANES, feat, LANES), bf16),
            vmem((2, feat, hid), bf16),
            vmem((hid, 2 * half_out), bf16),
            vmem((samples, block_rows, LANES), bf16),
            vmem((groups, block_rows, LANES), bf16),
            vmem((first, block_rows, LANES), bf16),
            vmem((late, block_rows, LANES), bf16),
            vmem((first, block_rows, LANES), bf16),
            vmem((late, block_rows, LANES), bf16),
            vmem((1, LANES), i32),
            vmem((groups, 1, LANES), i32),
            vmem((tile, feat), bf16),
            vmem((tile, feat), bf16),
            vmem((tile, hid), f32),
            vmem((tile, hid), bf16),
            vmem((samples, BLOCK, half_out), bf16),
            *[vmem((samples, BLOCK, size), bf16) for _, size in outs],
            *[vmem((samples, BLOCK, size), bf16) for _, size in outs],
            dma((6,)), dma((3,)), dma((4,)), dma((groups,)), dma((3,)), dma((parts,)), dma((parts,)),
        ],
        compiler_params=pltpu.CompilerParams(
            collective_id=0, has_side_effects=True, vmem_limit_bytes=60 * 1024 * 1024
        ),
    )(
        dest_seq, dest_slot, counts, win_ids, b_first, b_second, encoded.T, w_first, w_second,
    )


def solution(mesh):
    placed = (
        P("dp", "tensor"), P("dp"), P("dp", None), P("dp"), P("dp"),
        P(None, "tensor"), P("tensor"), P("tensor", None), P("tensor"),
    )
    return jax.shard_map(
        shards, mesh=mesh, in_specs=placed, out_specs=P("dp", "tensor"), check_vma=False
    )
```

```python
import functools
import math

import jax
import jax.numpy as jnp
from jax import lax
from jax.experimental import pallas as pl
from jax.experimental.pallas import tpu as pltpu
from jax.sharding import PartitionSpec as P

BLOCK = 32
LANES = 128
WIDE = 512
MESH = pl.DeviceIdType.MESH
UNROLL_MAX = 16
scope = jax.named_scope


def loop(count, body):
    if count <= UNROLL_MAX:
        for i in range(count):
            body(i)
    else:

        @pl.loop(0, count)
        def _(i):
            body(i)


def col_chunks(lo, hi, step):
    return [(at, min(step, hi - at)) for at in range(lo, hi, step)]


def gelu(x):
    c0 = math.sqrt(2.0 / math.pi)
    half = 0.5 * x
    return half + half * jnp.tanh(x * (c0 + (c0 * 0.044715) * (x * x)))


def settle(ref, sem):
    pltpu.make_async_copy(ref, ref, sem).wait()


def exchange_masks(groups):
    quarter, half = groups // 4, groups // 2
    bits = quarter.bit_length() - 1
    plane = [int(format(g, f"0{bits}b")[::-1], 2) if bits else 0 for g in range(quarter)]
    near = [m for m in plane] + [quarter + m for m in plane]
    far = [half + z * quarter + m for m in plane for z in (1, 0)]
    return near + far


def flip(me, mask, groups):
    total, bit = 0, 1
    while bit < groups:
        own = lax.rem(me // bit, 2)
        total = total + bit * ((1 - own) if mask & bit else own)
        bit *= 2
    return total


def kernel(
    dims,
    seq_h, slot_h, cnt_h, win_h, b1_h, b2_h, enc_h, w1_h, w2_h,
    out_v,
    seq_s, slot_s, cnt_s, win_v, b1_v, b2_v, val_s, pick_s, rank_s,
    enc, w1, w2, pooled, outgo, arr_a, arr_b, sib_a, sib_b, route_src, routes,
    x_mine, x_sib, pre, hidden, keep, *rest,
):
    groups, samples, cap, feat, parts = dims
    part_out, part_in = rest[:parts], rest[parts : 2 * parts]
    small_sem, load_sem, send_sem, recv_sem, group_sem, psend_sem, precv_sem = rest[2 * parts :]
    full = feat // LANES
    rem = feat - full * LANES
    wide = full * LANES
    hid = w1.shape[2]
    half_out = b2_v.shape[0]
    first = arr_a.shape[0]
    ranks = samples // 2
    tile = ranks * BLOCK
    me = lax.axis_index("dp")
    core = lax.axis_index("tensor")
    other = 1 - core
    masks = exchange_masks(groups)
    peers = [flip(me, mask, groups) for mask in masks]
    half = groups // 2
    order = [*range(half // 2, half), *range(1, half // 2)]
    for lo, hi in ((half, first), (first, groups)):
        order += [*range(lo, hi, 2), *range(lo + 1, hi, 2)]
    depth = me // (groups // 4)
    inner = lax.rem((depth + 1) // 2, 2)

    barrier = pltpu.get_barrier_semaphore()
    for o in range(1, groups):
        pl.semaphore_signal(barrier, 1, device_id={"dp": peers[o]}, device_id_type=MESH)
    pl.semaphore_signal(barrier, 1, device_id={"tensor": other}, device_id_type=MESH)

    pairs = samples * cap // LANES
    enc_copies = [
        pltpu.make_async_copy(enc_h.at[lo : lo + size], enc.at[lo : lo + size], load_sem.at[0])
        for lo, size in col_chunks(0, feat, 144)
    ]
    small = [
        pltpu.make_async_copy(src, dst, small_sem.at[n])
        for n, (src, dst) in enumerate(
            [(seq_h, seq_s), (slot_h, slot_s), (cnt_h, cnt_s), (win_h, win_v), (b1_h, b1_v), (b2_h, b2_v)]
        )
    ]
    for copy in small[:4] + enc_copies + small[4:]:
        copy.start()
    w1_copies = [
        pltpu.make_async_copy(w1_h.at[pl.ds(pl.multiple_of(side * feat, 64), feat)], w1.at[n], load_sem.at[1])
        for n, side in enumerate((core, other))
    ]
    w2_copies = [
        pltpu.make_async_copy(
            w2_h.at[:, pl.ds(pl.multiple_of(side * half_out, LANES), half_out)],
            w2.at[:, n * half_out : (n + 1) * half_out], load_sem.at[2],
        )
        for n, side in enumerate((other, core))
    ]
    with scope("loadwait"):
        for copy in small[:4]:
            copy.wait()
        settle(enc, load_sem.at[0])
    for copy in w1_copies + w2_copies:
        copy.start()

    lane = lax.broadcasted_iota(jnp.int32, route_src.shape, 1)
    route = jnp.full(route_src.shape, -1, jnp.int32)
    for s in range(samples):
        route = jnp.where(lane == s, seq_s[s] * samples + slot_s[s], route)
    route_src[...] = route
    routes[0] = route

    per = LANES // cap
    tall = per * BLOCK
    row_at = lax.broadcasted_iota(jnp.int32, (tall, LANES), 0)
    lane_at = lax.broadcasted_iota(jnp.int32, (tall, LANES), 1)
    windows = lax.rem(row_at, BLOCK)
    slot_at = lane_at - row_at // BLOCK * cap

    def pool(pair):
        at = pair * per
        ids = jnp.concatenate([win_v[at + n : at + n + 1, :] for n in range(per)], axis=1)
        limit = jnp.full((tall, LANES), jnp.minimum(cnt_s[at], cap))
        for n in range(1, per):
            limit = jnp.where(row_at >= n * BLOCK, jnp.minimum(cnt_s[at + n], cap), limit)
        live = (slot_at >= 0) & (slot_at < limit)
        hot = jnp.where((ids == windows) & live, 1.0, 0.0)
        number = jnp.sum(hot, axis=1, keepdims=True)
        total = lax.dot_general(
            hot.astype(jnp.bfloat16), enc[:, pair * LANES : (pair + 1) * LANES], (((1,), (1,)), ((), ())),
            preferred_element_type=jnp.float32,
        )
        y = (total * (1.0 / jnp.maximum(number, 1.0))).astype(jnp.bfloat16)
        for n in range(per):
            rows = y[n * BLOCK : (n + 1) * BLOCK]
            for c in range(full):
                pooled[at + n, c * BLOCK : (c + 1) * BLOCK, :] = rows[:, c * LANES : (c + 1) * LANES]
            if rem:
                tail = rows[:, wide:]
                mid = BLOCK // 2
                pooled[at + n, full * BLOCK :, :] = jnp.concatenate([tail[:mid], tail[mid:]], axis=1)

    def pick(peer):
        chosen = jnp.int32(0)
        for s in range(1, samples):
            chosen = jnp.where(seq_s[s] == peer, jnp.int32(s), chosen)
        return pooled[chosen]

    def place(o, near_ref, late_ref):
        return near_ref.at[o] if o < first else late_ref.at[o - first]

    def swapped(o):
        if o < half:
            return o, peers[o]
        low = o - (o - half) % 2
        lead = inner if o == low else 1 - inner
        return low + lead, lead * peers[low + 1] + (1 - lead) * peers[low]

    def send(o):
        slot, peer = swapped(o)
        home, at = (arr_a, slot) if o < first else (arr_b, slot - first)
        return pltpu.make_async_remote_copy(
            src_ref=outgo.at[slot], dst_ref=home.at[at], send_sem=send_sem.at[0], recv_sem=recv_sem.at[slot],
            device_id={"dp": peer}, device_id_type=MESH,
        )

    def data_copy(o):
        return pltpu.make_async_remote_copy(
            src_ref=outgo.at[o], dst_ref=place(o, arr_a, arr_b), send_sem=send_sem.at[0], recv_sem=recv_sem.at[o],
            device_id={"dp": peers[o]}, device_id_type=MESH,
        )

    def route_copy(o):
        return pltpu.make_async_remote_copy(
            src_ref=route_src, dst_ref=routes.at[o], send_sem=send_sem.at[1], recv_sem=group_sem.at[0],
            device_id={"dp": peers[o]}, device_id_type=MESH,
        )

    def forward(o):
        late_slot = int(o >= first)
        return pltpu.make_async_remote_copy(
            src_ref=place(o, arr_a, arr_b), dst_ref=place(o, sib_a, sib_b),
            send_sem=send_sem.at[2 + late_slot], recv_sem=group_sem.at[1 + late_slot],
            device_id={"tensor": other}, device_id_type=MESH,
        )

    with scope("pool"):
        for pair in range(pairs):
            pool(pair)

    def fill(o):
        slot, peer = swapped(o)
        outgo[slot] = pick(peer)

    ahead = 2
    for o in order[:ahead]:
        fill(o)
    with scope("barrier"):
        pl.semaphore_wait(barrier, groups)
    with scope("stage"):
        for o in order:
            route_copy(o).start()
        for n, o in enumerate(order[: first - 1]):
            fill(order[n + ahead])
            send(o).start()
        for o in order[first - 1 + ahead :]:
            fill(o)
        arr_a[0] = pick(me)

        @pl.when(core == 0)
        def _():
            for o in order[first - 1 :]:
                send(o).start()

        forward(0).start()

    with scope("routewait"):
        settle(routes.at[1:], group_sem.at[0])
    base = me * samples
    seen = jnp.int32(0)
    for o in range(groups):
        row = routes[o]
        hit = (row >= base) & (row < base + samples)
        value = jnp.sum(jnp.where(hit, row - base + 1, 0))
        val_s[o] = value
        val_s[groups + o] = seen
        seen = seen + jnp.minimum(value, 1)

    def find(r):
        at, spot = jnp.int32(0), jnp.int32(0)
        for o in range(groups):
            value, before = val_s[o], val_s[groups + o]
            at = jnp.where((value > 0) & (before == r), o, at)
            spot = jnp.where(value == r + 1, before, spot)
        pick_s[r] = at
        rank_s[r] = jnp.minimum(spot, samples - 1)

    with scope("picks"):
        loop(samples, find)

    def arrive(o):
        with scope(f"arr{o}"):
            data_copy(o).wait_recv()
        forward(o).start()

    def unpack(dst, r, block):
        lo = r * BLOCK if isinstance(r, int) else pl.multiple_of(r * BLOCK, BLOCK)
        for c in range(full):
            dst[pl.ds(lo, BLOCK), c * LANES : (c + 1) * LANES] = block[c * BLOCK : (c + 1) * BLOCK]
        if rem:
            mid = BLOCK // 2
            tail = block[full * BLOCK :]
            dst[pl.ds(lo, mid), wide:] = tail[:, :rem]
            dst[pl.ds(lo + mid, mid), wide:] = tail[:, rem:]

    def early(dst, ref):
        def one(r):
            unpack(dst, r, ref[jnp.minimum(pick_s[r], first - 1)])

        loop(ranks, one)

    def late(dst, ref, ref_late):
        def one(r):
            at = pick_s[ranks + r]
            a = ref[jnp.minimum(at, first - 1)]
            b = ref_late[jnp.maximum(at - first, 0)]
            unpack(dst, r, jnp.where(at < first, a, b))

        loop(ranks, one)

    step = min(256, tile)

    def over_rows(body):
        if tile == step:
            body(slice(0, step), 0)
        else:

            @pl.loop(0, tile // step)
            def _(m):
                body(pl.ds(pl.multiple_of(m * step, step), step), m * (step // BLOCK))

    up_chunks = col_chunks(0, hid, 768)

    def mine_part(rows, _):
        for lo, size in up_chunks:
            pre[rows, lo : lo + size] = jnp.dot(
                x_mine[rows, :], w1[0, :, lo : lo + size], preferred_element_type=jnp.float32
            )

    def sib_part(rows, _):
        for lo, size in up_chunks:
            acc = jnp.dot(x_sib[rows, :], w1[1, :, lo : lo + size], preferred_element_type=jnp.float32)
            acc = acc + pre[rows, lo : lo + size] + b1_v[lo : lo + size]
            hidden[rows, lo : lo + size] = gelu(acc).astype(jnp.bfloat16)

    outs = col_chunks(0, half_out, WIDE)
    even = half_out // 256 * 256
    spans = col_chunks(0, even, WIDE)
    if even < half_out:
        spans = spans + [(even, 256)]
    spans = spans + col_chunks(sum(spans[-1]), 2 * half_out, WIDE)

    def down(which, lo, size):
        def body(rows, at):
            y = jnp.dot(
                hidden[rows, :], w2[:, lo : lo + size], preferred_element_type=jnp.float32
            ).astype(jnp.bfloat16)
            for n, (start, width) in enumerate(outs):
                begin, end = max(lo, start), min(lo + size, start + width)
                if begin < end:
                    for r in range(step // BLOCK):
                        part_out[n][which * ranks + at + r, :, begin - start : end - start] = y[
                            r * BLOCK : (r + 1) * BLOCK, begin - lo : end - lo
                        ]
            begin = max(lo, half_out)
            if begin < lo + size:
                for r in range(step // BLOCK):
                    keep[which * ranks + at + r, :, begin - half_out : lo + size - half_out] = y[
                        r * BLOCK : (r + 1) * BLOCK, begin - lo :
                    ]

        over_rows(body)

    def part_copy(which, n):
        span = pl.ds(which * ranks, ranks)
        return pltpu.make_async_remote_copy(
            src_ref=part_out[n].at[span], dst_ref=part_in[n].at[span],
            send_sem=psend_sem.at[n], recv_sem=precv_sem.at[n],
            device_id={"tensor": other}, device_id_type=MESH,
        )

    def project(which):
        with scope(f"send{which}"):
            for lo, size in spans:
                if lo < half_out:
                    down(which, lo, size)
        for n in range(parts):
            part_copy(which, n).start()
        with scope(f"keep{which}"):
            for lo, size in spans:
                if lo >= half_out:
                    down(which, lo, size)

    for o in range(1, 8):
        arrive(o)

    @pl.when(core == 1)
    def _():
        for o in order[first - 1 :]:
            send(o).start()

    for o in range(8, first):
        arrive(o)

    with scope("fwdA"):
        settle(sib_a, group_sem.at[1])
    with scope("xA"):
        early(x_mine, arr_a)
        early(x_sib, sib_a)
    with scope("w1wait"):
        settle(w1, load_sem.at[1])
        for copy in small[4:]:
            copy.wait()
    with scope("upA"):
        over_rows(mine_part)
        over_rows(sib_part)
    with scope("w2wait"):
        settle(w2, load_sem.at[2])
    project(0)
    for o in range(first, groups):
        arrive(o)
    with scope("xBm"):
        late(x_mine, arr_a, arr_b)
    with scope("upBm"):
        over_rows(mine_part)
    with scope("fwdB"):
        settle(sib_b, group_sem.at[2])
    with scope("xBs"):
        late(x_sib, sib_a, sib_b)
    with scope("upBs"):
        over_rows(sib_part)
    project(1)
    for n, (lo, size) in enumerate(outs):
        with scope(f"pwait{n}"):
            settle(part_in[n], precv_sem.at[n])

        def finish(k):
            r = rank_s[k]
            rows = pl.ds(k * BLOCK if isinstance(k, int) else pl.multiple_of(k * BLOCK, BLOCK), BLOCK)
            both = keep[r, :, lo : lo + size].astype(jnp.float32) + part_in[n][r].astype(jnp.float32)
            out_v[rows, lo : lo + size] = (both + b2_v[lo : lo + size]).astype(jnp.bfloat16)

        with scope(f"finish{n}"):
            loop(samples, finish)
    with scope("drain"):
        settle(arr_a, send_sem.at[2])
        settle(arr_b, send_sem.at[3])
        settle(outgo.at[1:], send_sem.at[0])
        settle(routes.at[1:], send_sem.at[1])
        for n in range(parts):
            settle(part_out[n], psend_sem.at[n])


def shards(encoded, counts, win_ids, dest_seq, dest_slot, w_first, b_first, w_second, b_second):
    samples, cap = win_ids.shape
    feat = encoded.shape[1]
    groups = lax.axis_size("dp")
    hid = w_first.shape[1]
    half_out = b_second.shape[0]
    rows = samples * BLOCK
    tile = rows // 2
    block_rows = BLOCK * feat // LANES
    outs = col_chunks(0, half_out, WIDE)
    parts = len(outs)
    late = samples // 2
    first = groups - late
    hbm = pl.BlockSpec(memory_space=pltpu.HBM)
    bf16, f32, i32 = jnp.bfloat16, jnp.float32, jnp.int32
    vmem, smem, dma = pltpu.VMEM, pltpu.SMEM, pltpu.SemaphoreType.DMA
    return pl.pallas_call(
        functools.partial(kernel, (groups, samples, cap, feat, parts)),
        out_shape=vmem((rows, half_out), bf16),
        in_specs=[hbm] * 9,
        out_specs=pl.BlockSpec(memory_space=pltpu.VMEM),
        scratch_shapes=[
            smem((samples,), i32), smem((samples,), i32), smem((samples,), i32),
            vmem((samples, cap), i32), vmem((hid,), f32), vmem((half_out,), f32),
            smem((2 * groups,), i32), smem((samples,), i32), smem((samples,), i32),
            vmem((feat, samples * cap), bf16),
            vmem((2, feat, hid), bf16),
            vmem((hid, 2 * half_out), bf16),
            vmem((samples, block_rows, LANES), bf16),
            vmem((groups, block_rows, LANES), bf16),
            vmem((first, block_rows, LANES), bf16),
            vmem((late, block_rows, LANES), bf16),
            vmem((first, block_rows, LANES), bf16),
            vmem((late, block_rows, LANES), bf16),
            vmem((1, LANES), i32),
            vmem((groups, 1, LANES), i32),
            vmem((tile, feat), bf16),
            vmem((tile, feat), bf16),
            vmem((tile, hid), f32),
            vmem((tile, hid), bf16),
            vmem((samples, BLOCK, half_out), bf16),
            *[vmem((samples, BLOCK, size), bf16) for _, size in outs],
            *[vmem((samples, BLOCK, size), bf16) for _, size in outs],
            dma((6,)), dma((3,)), dma((4,)), dma((groups,)), dma((3,)), dma((parts,)), dma((parts,)),
        ],
        compiler_params=pltpu.CompilerParams(
            collective_id=0, has_side_effects=True, vmem_limit_bytes=60 * 1024 * 1024
        ),
    )(
        dest_seq, dest_slot, counts, win_ids, b_first, b_second, encoded.T, w_first, w_second,
    )


def solution(mesh):
    placed = (
        P("dp", "tensor"), P("dp"), P("dp", None), P("dp"), P("dp"),
        P(None, "tensor"), P("tensor"), P("tensor", None), P("tensor"),
    )
    return jax.shard_map(
        shards, mesh=mesh, in_specs=placed, out_specs=P("dp", "tensor"), check_vma=False
    )
```

```python
import functools
import math

import jax
import jax.numpy as jnp
from jax import lax
from jax.experimental import pallas as pl
from jax.experimental.pallas import tpu as pltpu
from jax.sharding import PartitionSpec as P

BLOCK = 32
LANES = 128
WIDE = 512
MESH = pl.DeviceIdType.MESH
UNROLL_MAX = 16
scope = jax.named_scope


def loop(count, body):
    if count <= UNROLL_MAX:
        for i in range(count):
            body(i)
    else:

        @pl.loop(0, count)
        def _(i):
            body(i)


def col_chunks(lo, hi, step):
    return [(at, min(step, hi - at)) for at in range(lo, hi, step)]


def gelu(x):
    c0 = math.sqrt(2.0 / math.pi)
    half = 0.5 * x
    return half + half * jnp.tanh(x * (c0 + (c0 * 0.044715) * (x * x)))


def settle(ref, sem):
    pltpu.make_async_copy(ref, ref, sem).wait()


def exchange_masks(groups):
    quarter, half = groups // 4, groups // 2
    bits = quarter.bit_length() - 1
    plane = [int(format(g, f"0{bits}b")[::-1], 2) if bits else 0 for g in range(quarter)]
    near = [m for m in plane] + [quarter + m for m in plane]
    far = [half + z * quarter + m for m in plane for z in (1, 0)]
    return near + far


def flip(me, mask, groups):
    total, bit = 0, 1
    while bit < groups:
        own = lax.rem(me // bit, 2)
        total = total + bit * ((1 - own) if mask & bit else own)
        bit *= 2
    return total


def kernel(
    dims,
    seq_h, slot_h, cnt_h, win_h, b1_h, b2_h, enc_h, w1_h, w2_h,
    out_v,
    seq_s, slot_s, cnt_s, win_v, b1_v, b2_v, val_s, pick_s, rank_s,
    enc, w1, w2, pooled, outgo, arr_a, arr_b, sib_a, sib_b, route_src, routes,
    x_mine, x_sib, pre, hidden, keep, *rest,
):
    groups, samples, cap, feat, parts = dims
    part_out, part_in = rest[:parts], rest[parts : 2 * parts]
    ready_sem, small_sem, load_sem, send_sem, recv_sem, group_sem, psend_sem, precv_sem = rest[2 * parts :]
    full = feat // LANES
    rem = feat - full * LANES
    wide = full * LANES
    hid = w1.shape[2]
    half_out = b2_v.shape[0]
    first = arr_a.shape[0]
    ranks = samples // 2
    tile = ranks * BLOCK
    me = lax.axis_index("dp")
    core = lax.axis_index("tensor")
    other = 1 - core
    masks = exchange_masks(groups)
    peers = [flip(me, mask, groups) for mask in masks]
    half = groups // 2
    near = [*range(half // 2, half), *range(1, half // 2)]
    far_a = [*range(half, first, 2), *range(half + 1, first, 2)]
    far_b = [*range(first, groups, 2), *range(first + 1, groups, 2)]
    side = me // half
    above = [lax.rem(me // (1 << max(mask.bit_length() - 1, 0)), 2) == 0 for mask in masks]
    depth = me // (groups // 4)
    inner = lax.rem((depth + 1) // 2, 2)

    barrier = pltpu.get_barrier_semaphore()
    pl.semaphore_signal(barrier, 1, device_id={"tensor": other}, device_id_type=MESH)
    for o in range(1, half):

        @pl.when(above[o] | (side == 0))
        def _():
            pl.semaphore_signal(barrier, 1, device_id={"dp": peers[o]}, device_id_type=MESH)

    for o in range(half, groups):
        pl.semaphore_signal(barrier, 1, device_id={"dp": peers[o]}, device_id_type=MESH)

    def meet():
        pl.semaphore_wait(barrier, side * (me + 1) + (1 - side) * groups)

        @pl.when(side == 1)
        def _():
            for o in range(1, half):

                @pl.when(jnp.logical_not(above[o]))
                def _():
                    pl.semaphore_signal(ready_sem.at[0], 1, device_id={"dp": peers[o]}, device_id_type=MESH)

    pairs = samples * cap // LANES
    enc_copies = [
        pltpu.make_async_copy(enc_h.at[lo : lo + size], enc.at[lo : lo + size], load_sem.at[0])
        for lo, size in col_chunks(0, feat, 144)
    ]
    small = [
        pltpu.make_async_copy(src, dst, small_sem.at[n])
        for n, (src, dst) in enumerate(
            [(seq_h, seq_s), (slot_h, slot_s), (cnt_h, cnt_s), (win_h, win_v), (b1_h, b1_v), (b2_h, b2_v)]
        )
    ]
    for copy in small[:4] + enc_copies + small[4:]:
        copy.start()
    w1_copies = [
        pltpu.make_async_copy(w1_h.at[pl.ds(pl.multiple_of(side * feat, 64), feat)], w1.at[n], load_sem.at[1])
        for n, side in enumerate((core, other))
    ]
    w2_copies = [
        pltpu.make_async_copy(
            w2_h.at[:, pl.ds(pl.multiple_of(side * half_out, LANES), half_out)],
            w2.at[:, n * half_out : (n + 1) * half_out], load_sem.at[2],
        )
        for n, side in enumerate((other, core))
    ]

    @pl.when(depth == 3)
    def _():
        meet()

    with scope("loadwait"):
        for copy in small[:4]:
            copy.wait()
        settle(enc, load_sem.at[0])
    for copy in w1_copies + w2_copies:
        copy.start()

    lane = lax.broadcasted_iota(jnp.int32, route_src.shape, 1)
    route = jnp.full(route_src.shape, -1, jnp.int32)
    for s in range(samples):
        route = jnp.where(lane == s, seq_s[s] * samples + slot_s[s], route)
    route_src[...] = route
    routes[0] = route

    per = LANES // cap
    tall = per * BLOCK
    row_at = lax.broadcasted_iota(jnp.int32, (tall, LANES), 0)
    lane_at = lax.broadcasted_iota(jnp.int32, (tall, LANES), 1)
    windows = lax.rem(row_at, BLOCK)
    slot_at = lane_at - row_at // BLOCK * cap

    def pool(pair):
        at = pair * per
        ids = jnp.concatenate([win_v[at + n : at + n + 1, :] for n in range(per)], axis=1)
        limit = jnp.full((tall, LANES), jnp.minimum(cnt_s[at], cap))
        for n in range(1, per):
            limit = jnp.where(row_at >= n * BLOCK, jnp.minimum(cnt_s[at + n], cap), limit)
        live = (slot_at >= 0) & (slot_at < limit)
        hot = jnp.where((ids == windows) & live, 1.0, 0.0)
        number = jnp.sum(hot, axis=1, keepdims=True)
        total = lax.dot_general(
            hot.astype(jnp.bfloat16), enc[:, pair * LANES : (pair + 1) * LANES], (((1,), (1,)), ((), ())),
            preferred_element_type=jnp.float32,
        )
        y = (total * (1.0 / jnp.maximum(number, 1.0))).astype(jnp.bfloat16)
        for n in range(per):
            rows = y[n * BLOCK : (n + 1) * BLOCK]
            for c in range(full):
                pooled[at + n, c * BLOCK : (c + 1) * BLOCK, :] = rows[:, c * LANES : (c + 1) * LANES]
            if rem:
                tail = rows[:, wide:]
                mid = BLOCK // 2
                pooled[at + n, full * BLOCK :, :] = jnp.concatenate([tail[:mid], tail[mid:]], axis=1)

    def pick(peer):
        chosen = jnp.int32(0)
        for s in range(1, samples):
            chosen = jnp.where(seq_s[s] == peer, jnp.int32(s), chosen)
        return pooled[chosen]

    def place(o, near_ref, late_ref):
        return near_ref.at[o] if o < first else late_ref.at[o - first]

    def swapped(o):
        if o < half:
            return o, peers[o]
        low = o - (o - half) % 2
        lead = inner if o == low else 1 - inner
        return low + lead, lead * peers[low + 1] + (1 - lead) * peers[low]

    def send(o):
        slot, peer = swapped(o)
        home, at = (arr_a, slot) if o < first else (arr_b, slot - first)
        return pltpu.make_async_remote_copy(
            src_ref=outgo.at[slot], dst_ref=home.at[at], send_sem=send_sem.at[0], recv_sem=recv_sem.at[slot],
            device_id={"dp": peer}, device_id_type=MESH,
        )

    def data_copy(o):
        return pltpu.make_async_remote_copy(
            src_ref=outgo.at[o], dst_ref=place(o, arr_a, arr_b), send_sem=send_sem.at[0], recv_sem=recv_sem.at[o],
            device_id={"dp": peers[o]}, device_id_type=MESH,
        )

    def route_copy(o):
        return pltpu.make_async_remote_copy(
            src_ref=route_src, dst_ref=routes.at[o], send_sem=send_sem.at[1], recv_sem=group_sem.at[0],
            device_id={"dp": peers[o]}, device_id_type=MESH,
        )

    def forward(o):
        late_slot = int(o >= first)
        return pltpu.make_async_remote_copy(
            src_ref=place(o, arr_a, arr_b), dst_ref=place(o, sib_a, sib_b),
            send_sem=send_sem.at[2 + late_slot], recv_sem=group_sem.at[1 + late_slot],
            device_id={"tensor": other}, device_id_type=MESH,
        )

    with scope("pool"):
        for pair in range(pairs):
            pool(pair)

    def fill(o):
        slot, peer = swapped(o)
        outgo[slot] = pick(peer)

    def launch(slots):
        for o in slots:
            send(o).start()

    for o in far_a:
        fill(o)
    with scope("barrier"):

        @pl.when(depth != 3)
        def _():
            meet()

    with scope("stage"):

        for o in range(half, groups):
            route_copy(o).start()

        @pl.when(side == 1)
        def _():
            launch(far_a)

        for o in near:

            @pl.when(jnp.logical_not(above[o]) | (side == 0))
            def _():
                route_copy(o).start()

        for o in far_b + near:
            fill(o)

        arr_a[0] = pick(me)
        for o in near:

            @pl.when(jnp.logical_not(above[o]) | (side == 0))
            def _():
                send(o).start()

        forward(0).start()
    with scope("nearready"):

        @pl.when((side == 1) & (me < groups - 1))
        def _():
            pl.semaphore_wait(ready_sem.at[0], groups - 1 - me)

    for slots, copy in ((near, route_copy), (near, send)):
        for o in slots:

            @pl.when(above[o] & (side == 1))
            def _():
                copy(o).start()

    @pl.when(side == 0)
    def _():
        launch(far_a)

    @pl.when(core == 0)
    def _():
        launch(far_b)

    def arrive(o):
        with scope(f"arr{o}"):
            data_copy(o).wait_recv()
        forward(o).start()

    def unpack(dst, r, block):
        lo = r * BLOCK if isinstance(r, int) else pl.multiple_of(r * BLOCK, BLOCK)
        for c in range(full):
            dst[pl.ds(lo, BLOCK), c * LANES : (c + 1) * LANES] = block[c * BLOCK : (c + 1) * BLOCK]
        if rem:
            mid = BLOCK // 2
            tail = block[full * BLOCK :]
            dst[pl.ds(lo, mid), wide:] = tail[:, :rem]
            dst[pl.ds(lo + mid, mid), wide:] = tail[:, rem:]

    def early(dst, ref):
        def one(r):
            unpack(dst, r, ref[jnp.minimum(pick_s[r], first - 1)])

        loop(ranks, one)

    def late(dst, ref, ref_late):
        def one(r):
            at = pick_s[ranks + r]
            a = ref[jnp.minimum(at, first - 1)]
            b = ref_late[jnp.maximum(at - first, 0)]
            unpack(dst, r, jnp.where(at < first, a, b))

        loop(ranks, one)

    step = min(256, tile)

    def over_rows(body):
        if tile == step:
            body(slice(0, step), 0)
        else:

            @pl.loop(0, tile // step)
            def _(m):
                body(pl.ds(pl.multiple_of(m * step, step), step), m * (step // BLOCK))

    up_chunks = col_chunks(0, hid, 768)

    def mine_part(rows, _):
        for lo, size in up_chunks:
            pre[rows, lo : lo + size] = jnp.dot(
                x_mine[rows, :], w1[0, :, lo : lo + size], preferred_element_type=jnp.float32
            )

    def sib_part(rows, _):
        for lo, size in up_chunks:
            acc = jnp.dot(x_sib[rows, :], w1[1, :, lo : lo + size], preferred_element_type=jnp.float32)
            acc = acc + pre[rows, lo : lo + size] + b1_v[lo : lo + size]
            hidden[rows, lo : lo + size] = gelu(acc).astype(jnp.bfloat16)

    outs = col_chunks(0, half_out, WIDE)
    even = half_out // 256 * 256
    spans = col_chunks(0, even, WIDE)
    if even < half_out:
        spans = spans + [(even, 256)]
    spans = spans + col_chunks(sum(spans[-1]), 2 * half_out, WIDE)

    def down(which, lo, size):
        def body(rows, at):
            y = jnp.dot(
                hidden[rows, :], w2[:, lo : lo + size], preferred_element_type=jnp.float32
            ).astype(jnp.bfloat16)
            for n, (start, width) in enumerate(outs):
                begin, end = max(lo, start), min(lo + size, start + width)
                if begin < end:
                    for r in range(step // BLOCK):
                        part_out[n][which * ranks + at + r, :, begin - start : end - start] = y[
                            r * BLOCK : (r + 1) * BLOCK, begin - lo : end - lo
                        ]
            begin = max(lo, half_out)
            if begin < lo + size:
                for r in range(step // BLOCK):
                    keep[which * ranks + at + r, :, begin - half_out : lo + size - half_out] = y[
                        r * BLOCK : (r + 1) * BLOCK, begin - lo :
                    ]

        over_rows(body)

    def part_copy(which, n):
        span = pl.ds(which * ranks, ranks)
        return pltpu.make_async_remote_copy(
            src_ref=part_out[n].at[span], dst_ref=part_in[n].at[span],
            send_sem=psend_sem.at[n], recv_sem=precv_sem.at[n],
            device_id={"tensor": other}, device_id_type=MESH,
        )

    def project(which):
        with scope(f"send{which}"):
            for lo, size in spans:
                if lo < half_out:
                    down(which, lo, size)
        for n in range(parts):
            part_copy(which, n).start()
        with scope(f"keep{which}"):
            for lo, size in spans:
                if lo >= half_out:
                    down(which, lo, size)

    for o in range(1, half):
        arrive(o)

    @pl.when(core == 1)
    def _():
        launch(far_b)

    for o in range(half, first):
        arrive(o)

    with scope("routewait"):
        settle(routes.at[1:], group_sem.at[0])
    base = me * samples
    seen = jnp.int32(0)
    for o in range(groups):
        row = routes[o]
        hit = (row >= base) & (row < base + samples)
        value = jnp.sum(jnp.where(hit, row - base + 1, 0))
        val_s[o] = value
        val_s[groups + o] = seen
        seen = seen + jnp.minimum(value, 1)

    def find(r):
        at, spot = jnp.int32(0), jnp.int32(0)
        for o in range(groups):
            value, before = val_s[o], val_s[groups + o]
            at = jnp.where((value > 0) & (before == r), o, at)
            spot = jnp.where(value == r + 1, before, spot)
        pick_s[r] = at
        rank_s[r] = jnp.minimum(spot, samples - 1)

    with scope("picks"):
        loop(samples, find)
    with scope("fwdA"):
        settle(sib_a, group_sem.at[1])
    with scope("xA"):
        early(x_mine, arr_a)
        early(x_sib, sib_a)
    with scope("w1wait"):
        settle(w1, load_sem.at[1])
        for copy in small[4:]:
            copy.wait()
    with scope("upA"):
        over_rows(mine_part)
        over_rows(sib_part)
    with scope("w2wait"):
        settle(w2, load_sem.at[2])
    project(0)
    for o in range(first, groups):
        arrive(o)
    with scope("xBm"):
        late(x_mine, arr_a, arr_b)
    with scope("upBm"):
        over_rows(mine_part)
    with scope("fwdB"):
        settle(sib_b, group_sem.at[2])
    with scope("xBs"):
        late(x_sib, sib_a, sib_b)
    with scope("upBs"):
        over_rows(sib_part)
    project(1)
    for n, (lo, size) in enumerate(outs):
        with scope(f"pwait{n}"):
            settle(part_in[n], precv_sem.at[n])

        def finish(k):
            r = rank_s[k]
            rows = pl.ds(k * BLOCK if isinstance(k, int) else pl.multiple_of(k * BLOCK, BLOCK), BLOCK)
            both = keep[r, :, lo : lo + size].astype(jnp.float32) + part_in[n][r].astype(jnp.float32)
            out_v[rows, lo : lo + size] = (both + b2_v[lo : lo + size]).astype(jnp.bfloat16)

        with scope(f"finish{n}"):
            loop(samples, finish)
    with scope("drain"):
        settle(arr_a, send_sem.at[2])
        settle(arr_b, send_sem.at[3])
        settle(outgo.at[1:], send_sem.at[0])
        settle(routes.at[1:], send_sem.at[1])
        for n in range(parts):
            settle(part_out[n], psend_sem.at[n])


def shards(encoded, counts, win_ids, dest_seq, dest_slot, w_first, b_first, w_second, b_second):
    samples, cap = win_ids.shape
    feat = encoded.shape[1]
    groups = lax.axis_size("dp")
    hid = w_first.shape[1]
    half_out = b_second.shape[0]
    rows = samples * BLOCK
    tile = rows // 2
    block_rows = BLOCK * feat // LANES
    outs = col_chunks(0, half_out, WIDE)
    parts = len(outs)
    late = samples // 2
    first = groups - late
    hbm = pl.BlockSpec(memory_space=pltpu.HBM)
    bf16, f32, i32 = jnp.bfloat16, jnp.float32, jnp.int32
    vmem, smem, dma = pltpu.VMEM, pltpu.SMEM, pltpu.SemaphoreType.DMA
    return pl.pallas_call(
        functools.partial(kernel, (groups, samples, cap, feat, parts)),
        out_shape=vmem((rows, half_out), bf16),
        in_specs=[hbm] * 9,
        out_specs=pl.BlockSpec(memory_space=pltpu.VMEM),
        scratch_shapes=[
            smem((samples,), i32), smem((samples,), i32), smem((samples,), i32),
            vmem((samples, cap), i32), vmem((hid,), f32), vmem((half_out,), f32),
            smem((2 * groups,), i32), smem((samples,), i32), smem((samples,), i32),
            vmem((feat, samples * cap), bf16),
            vmem((2, feat, hid), bf16),
            vmem((hid, 2 * half_out), bf16),
            vmem((samples, block_rows, LANES), bf16),
            vmem((groups, block_rows, LANES), bf16),
            vmem((first, block_rows, LANES), bf16),
            vmem((late, block_rows, LANES), bf16),
            vmem((first, block_rows, LANES), bf16),
            vmem((late, block_rows, LANES), bf16),
            vmem((1, LANES), i32),
            vmem((groups, 1, LANES), i32),
            vmem((tile, feat), bf16),
            vmem((tile, feat), bf16),
            vmem((tile, hid), f32),
            vmem((tile, hid), bf16),
            vmem((samples, BLOCK, half_out), bf16),
            *[vmem((samples, BLOCK, size), bf16) for _, size in outs],
            *[vmem((samples, BLOCK, size), bf16) for _, size in outs],
            pltpu.SemaphoreType.REGULAR((1,)), dma((6,)), dma((3,)), dma((4,)), dma((groups,)), dma((3,)), dma((parts,)), dma((parts,)),
        ],
        compiler_params=pltpu.CompilerParams(
            collective_id=0, has_side_effects=True, vmem_limit_bytes=60 * 1024 * 1024
        ),
    )(
        dest_seq, dest_slot, counts, win_ids, b_first, b_second, encoded.T, w_first, w_second,
    )


def solution(mesh):
    placed = (
        P("dp", "tensor"), P("dp"), P("dp", None), P("dp"), P("dp"),
        P(None, "tensor"), P("tensor"), P("tensor", None), P("tensor"),
    )
    return jax.shard_map(
        shards, mesh=mesh, in_specs=placed, out_specs=P("dp", "tensor"), check_vma=False
    )
```

```python
import functools
import math

import jax
import jax.numpy as jnp
from jax import lax
from jax.experimental import pallas as pl
from jax.experimental.pallas import tpu as pltpu
from jax.sharding import PartitionSpec as P

BLOCK = 32
LANES = 128
WIDE = 512
MESH = pl.DeviceIdType.MESH
UNROLL_MAX = 16
scope = jax.named_scope


def loop(count, body):
    if count <= UNROLL_MAX:
        for i in range(count):
            body(i)
    else:

        @pl.loop(0, count)
        def _(i):
            body(i)


def col_chunks(lo, hi, step):
    return [(at, min(step, hi - at)) for at in range(lo, hi, step)]


def gelu(x):
    c0 = math.sqrt(2.0 / math.pi)
    half = 0.5 * x
    return half + half * jnp.tanh(x * (c0 + (c0 * 0.044715) * (x * x)))


def settle(ref, sem):
    pltpu.make_async_copy(ref, ref, sem).wait()


def exchange_masks(groups):
    quarter, half = groups // 4, groups // 2
    bits = quarter.bit_length() - 1
    plane = [int(format(g, f"0{bits}b")[::-1], 2) if bits else 0 for g in range(quarter)]
    near = [m for m in plane] + [quarter + m for m in plane]
    far = [half + z * quarter + m for m in plane for z in (1, 0)]
    return near + far


def flip(me, mask, groups):
    total, bit = 0, 1
    while bit < groups:
        own = lax.rem(me // bit, 2)
        total = total + bit * ((1 - own) if mask & bit else own)
        bit *= 2
    return total


def kernel(
    dims,
    seq_h, slot_h, cnt_h, win_h, b1_h, b2_h, enc_h, w1_h, w2_h,
    out_v,
    seq_s, slot_s, cnt_s, win_v, b1_v, b2_v, val_s, pick_s, rank_s,
    enc, w1, w2, pooled, outgo, arr_a, arr_b, sib_a, sib_b, route_src, routes,
    x_mine, x_sib, pre, hidden, keep, *rest,
):
    groups, samples, cap, feat, parts = dims
    part_out, part_in = rest[:parts], rest[parts : 2 * parts]
    ready_sem, small_sem, load_sem, send_sem, recv_sem, group_sem, psend_sem, precv_sem = rest[2 * parts :]
    full = feat // LANES
    rem = feat - full * LANES
    wide = full * LANES
    hid = w1.shape[2]
    half_out = b2_v.shape[0]
    first = arr_a.shape[0]
    ranks = samples // 2
    tile = ranks * BLOCK
    me = lax.axis_index("dp")
    core = lax.axis_index("tensor")
    other = 1 - core
    masks = exchange_masks(groups)
    peers = [flip(me, mask, groups) for mask in masks]
    half = groups // 2
    near = [*range(half // 2, half), *range(1, half // 2)]
    far_a = [*range(half, first, 2), *range(half + 1, first, 2)]
    far_b = [*range(first, groups, 2), *range(first + 1, groups, 2)]
    side = me // half
    above = [lax.rem(me // (1 << max(mask.bit_length() - 1, 0)), 2) == 0 for mask in masks]
    depth = me // (groups // 4)
    inner = lax.rem((depth + 1) // 2, 2)

    barrier = pltpu.get_barrier_semaphore()
    pl.semaphore_signal(barrier, 1, device_id={"tensor": other}, device_id_type=MESH)
    for o in range(1, half):

        @pl.when(above[o] | (side == 0))
        def _():
            pl.semaphore_signal(barrier, 1, device_id={"dp": peers[o]}, device_id_type=MESH)

    for o in range(half, groups):
        pl.semaphore_signal(barrier, 1, device_id={"dp": peers[o]}, device_id_type=MESH)

    def meet():
        pl.semaphore_wait(barrier, side * (me + 1) + (1 - side) * groups)

        @pl.when(side == 1)
        def _():
            for o in range(1, half):

                @pl.when(jnp.logical_not(above[o]))
                def _():
                    pl.semaphore_signal(ready_sem.at[0], 1, device_id={"dp": peers[o]}, device_id_type=MESH)

    pairs = samples * cap // LANES
    enc_copies = [
        pltpu.make_async_copy(enc_h.at[lo : lo + size], enc.at[lo : lo + size], load_sem.at[0])
        for lo, size in col_chunks(0, feat, 144)
    ]
    small = [
        pltpu.make_async_copy(src, dst, small_sem.at[n])
        for n, (src, dst) in enumerate(
            [(seq_h, seq_s), (slot_h, slot_s), (cnt_h, cnt_s), (win_h, win_v), (b1_h, b1_v), (b2_h, b2_v)]
        )
    ]
    for copy in small[:4] + enc_copies + small[4:]:
        copy.start()
    w1_copies = [
        pltpu.make_async_copy(w1_h.at[pl.ds(pl.multiple_of(side * feat, 64), feat)], w1.at[n], load_sem.at[1])
        for n, side in enumerate((core, other))
    ]
    w2_copies = [
        pltpu.make_async_copy(
            w2_h.at[:, pl.ds(pl.multiple_of(side * half_out, LANES), half_out)],
            w2.at[:, n * half_out : (n + 1) * half_out], load_sem.at[2],
        )
        for n, side in enumerate((other, core))
    ]

    @pl.when(depth == 3)
    def _():
        meet()

    with scope("loadwait"):
        for copy in small[:4]:
            copy.wait()
        settle(enc, load_sem.at[0])
    for copy in w1_copies + w2_copies:
        copy.start()

    lane = lax.broadcasted_iota(jnp.int32, route_src.shape, 1)
    route = jnp.full(route_src.shape, -1, jnp.int32)
    for s in range(samples):
        route = jnp.where(lane == s, seq_s[s] * samples + slot_s[s], route)
    route_src[...] = route
    routes[0] = route

    per = LANES // cap
    tall = per * BLOCK
    row_at = lax.broadcasted_iota(jnp.int32, (tall, LANES), 0)
    lane_at = lax.broadcasted_iota(jnp.int32, (tall, LANES), 1)
    windows = lax.rem(row_at, BLOCK)
    slot_at = lane_at - row_at // BLOCK * cap

    def pool(pair):
        at = pair * per
        ids = jnp.concatenate([win_v[at + n : at + n + 1, :] for n in range(per)], axis=1)
        limit = jnp.full((tall, LANES), jnp.minimum(cnt_s[at], cap))
        for n in range(1, per):
            limit = jnp.where(row_at >= n * BLOCK, jnp.minimum(cnt_s[at + n], cap), limit)
        live = (slot_at >= 0) & (slot_at < limit)
        hot = jnp.where((ids == windows) & live, 1.0, 0.0)
        number = jnp.sum(hot, axis=1, keepdims=True)
        total = lax.dot_general(
            hot.astype(jnp.bfloat16), enc[:, pair * LANES : (pair + 1) * LANES], (((1,), (1,)), ((), ())),
            preferred_element_type=jnp.float32,
        )
        y = (total * (1.0 / jnp.maximum(number, 1.0))).astype(jnp.bfloat16)
        for n in range(per):
            rows = y[n * BLOCK : (n + 1) * BLOCK]
            for c in range(full):
                pooled[at + n, c * BLOCK : (c + 1) * BLOCK, :] = rows[:, c * LANES : (c + 1) * LANES]
            if rem:
                tail = rows[:, wide:]
                mid = BLOCK // 2
                pooled[at + n, full * BLOCK :, :] = jnp.concatenate([tail[:mid], tail[mid:]], axis=1)

    def pick(peer):
        chosen = jnp.int32(0)
        for s in range(1, samples):
            chosen = jnp.where(seq_s[s] == peer, jnp.int32(s), chosen)
        return pooled[chosen]

    def swapped(o):
        if o < half:
            return o, peers[o]
        low = o - (o - half) % 2
        lead = inner if o == low else 1 - inner
        return low + lead, lead * peers[low + 1] + (1 - lead) * peers[low]

    def send(o):
        slot, peer = swapped(o)
        home, at = (arr_a, slot) if o < first else (arr_b, slot - first)
        return pltpu.make_async_remote_copy(
            src_ref=outgo.at[slot], dst_ref=home.at[at], send_sem=send_sem.at[0], recv_sem=recv_sem.at[slot // 2],
            device_id={"dp": peer}, device_id_type=MESH,
        )

    def route_copy(o):
        return pltpu.make_async_remote_copy(
            src_ref=route_src, dst_ref=routes.at[o], send_sem=send_sem.at[1], recv_sem=group_sem.at[0],
            device_id={"dp": peers[o]}, device_id_type=MESH,
        )

    def span(lo, size, near_ref, late_ref):
        return near_ref.at[pl.ds(lo, size)] if lo < first else late_ref.at[pl.ds(lo - first, size)]

    def forward(lo, size):
        late_slot = int(lo >= first)
        return pltpu.make_async_remote_copy(
            src_ref=span(lo, size, arr_a, arr_b), dst_ref=span(lo, size, sib_a, sib_b),
            send_sem=send_sem.at[2 + late_slot], recv_sem=group_sem.at[1 + late_slot],
            device_id={"tensor": other}, device_id_type=MESH,
        )

    with scope("pool"):
        for pair in range(pairs):
            pool(pair)

    def fill(o):
        slot, peer = swapped(o)
        outgo[slot] = pick(peer)

    def launch(slots):
        for o in slots:
            send(o).start()

    for o in far_a:
        fill(o)
    with scope("barrier"):

        @pl.when(depth != 3)
        def _():
            meet()

    with scope("stage"):

        for o in range(half, groups):
            route_copy(o).start()

        @pl.when(side == 1)
        def _():
            launch(far_a)

        for o in near:

            @pl.when(jnp.logical_not(above[o]) | (side == 0))
            def _():
                route_copy(o).start()

        for o in far_b + near:
            fill(o)

        arr_a[0] = pick(me)
        for o in near:

            @pl.when(jnp.logical_not(above[o]) | (side == 0))
            def _():
                send(o).start()

        forward(0, 1).start()
    with scope("nearready"):

        @pl.when((side == 1) & (me < groups - 1))
        def _():
            pl.semaphore_wait(ready_sem.at[0], groups - 1 - me)

    for slots, copy in ((near, route_copy), (near, send)):
        for o in slots:

            @pl.when(above[o] & (side == 1))
            def _():
                copy(o).start()

    @pl.when(side == 0)
    def _():
        launch(far_a)

    @pl.when(core == 0)
    def _():
        launch(far_b)

    def arrive(lo, hi):
        for at in range(lo, hi, 2):
            start, size = (at, 2) if at else (1, 1)
            with scope(f"arr{at}"):
                settle(span(start, size, arr_a, arr_b), recv_sem.at[at // 2])
            forward(start, size).start()

    def unpack(dst, r, block):
        lo = r * BLOCK if isinstance(r, int) else pl.multiple_of(r * BLOCK, BLOCK)
        for c in range(full):
            dst[pl.ds(lo, BLOCK), c * LANES : (c + 1) * LANES] = block[c * BLOCK : (c + 1) * BLOCK]
        if rem:
            mid = BLOCK // 2
            tail = block[full * BLOCK :]
            dst[pl.ds(lo, mid), wide:] = tail[:, :rem]
            dst[pl.ds(lo + mid, mid), wide:] = tail[:, rem:]

    def early(dst, ref):
        def one(r):
            unpack(dst, r, ref[jnp.minimum(pick_s[r], first - 1)])

        loop(ranks, one)

    def late(dst, ref, ref_late):
        def one(r):
            at = pick_s[ranks + r]
            a = ref[jnp.minimum(at, first - 1)]
            b = ref_late[jnp.maximum(at - first, 0)]
            unpack(dst, r, jnp.where(at < first, a, b))

        loop(ranks, one)

    step = min(256, tile)

    def over_rows(body):
        if tile == step:
            body(slice(0, step), 0)
        else:

            @pl.loop(0, tile // step)
            def _(m):
                body(pl.ds(pl.multiple_of(m * step, step), step), m * (step // BLOCK))

    up_chunks = col_chunks(0, hid, 768)

    def mine_part(rows, _):
        for lo, size in up_chunks:
            pre[rows, lo : lo + size] = jnp.dot(
                x_mine[rows, :], w1[0, :, lo : lo + size], preferred_element_type=jnp.float32
            )

    def sib_part(rows, _):
        for lo, size in up_chunks:
            acc = jnp.dot(x_sib[rows, :], w1[1, :, lo : lo + size], preferred_element_type=jnp.float32)
            acc = acc + pre[rows, lo : lo + size] + b1_v[lo : lo + size]
            hidden[rows, lo : lo + size] = gelu(acc).astype(jnp.bfloat16)

    outs = col_chunks(0, half_out, WIDE)
    even = half_out // 256 * 256
    spans = col_chunks(0, even, WIDE)
    if even < half_out:
        spans = spans + [(even, 256)]
    spans = spans + col_chunks(sum(spans[-1]), 2 * half_out, WIDE)

    def down(which, lo, size):
        def body(rows, at):
            y = jnp.dot(
                hidden[rows, :], w2[:, lo : lo + size], preferred_element_type=jnp.float32
            ).astype(jnp.bfloat16)
            for n, (start, width) in enumerate(outs):
                begin, end = max(lo, start), min(lo + size, start + width)
                if begin < end:
                    for r in range(step // BLOCK):
                        part_out[n][which * ranks + at + r, :, begin - start : end - start] = y[
                            r * BLOCK : (r + 1) * BLOCK, begin - lo : end - lo
                        ]
            begin = max(lo, half_out)
            if begin < lo + size:
                for r in range(step // BLOCK):
                    keep[which * ranks + at + r, :, begin - half_out : lo + size - half_out] = y[
                        r * BLOCK : (r + 1) * BLOCK, begin - lo :
                    ]

        over_rows(body)

    def part_copy(which, n):
        span = pl.ds(which * ranks, ranks)
        return pltpu.make_async_remote_copy(
            src_ref=part_out[n].at[span], dst_ref=part_in[n].at[span],
            send_sem=psend_sem.at[n], recv_sem=precv_sem.at[n],
            device_id={"tensor": other}, device_id_type=MESH,
        )

    def project(which):
        with scope(f"send{which}"):
            for lo, size in spans:
                if lo < half_out:
                    down(which, lo, size)
        for n in range(parts):
            part_copy(which, n).start()
        with scope(f"keep{which}"):
            for lo, size in spans:
                if lo >= half_out:
                    down(which, lo, size)

    arrive(0, half)

    @pl.when(core == 1)
    def _():
        launch(far_b)

    arrive(half, first)

    with scope("routewait"):
        settle(routes.at[1:], group_sem.at[0])
    base = me * samples
    seen = jnp.int32(0)
    for o in range(groups):
        row = routes[o]
        hit = (row >= base) & (row < base + samples)
        value = jnp.sum(jnp.where(hit, row - base + 1, 0))
        val_s[o] = value
        val_s[groups + o] = seen
        seen = seen + jnp.minimum(value, 1)

    def find(r):
        at, spot = jnp.int32(0), jnp.int32(0)
        for o in range(groups):
            value, before = val_s[o], val_s[groups + o]
            at = jnp.where((value > 0) & (before == r), o, at)
            spot = jnp.where(value == r + 1, before, spot)
        pick_s[r] = at
        rank_s[r] = jnp.minimum(spot, samples - 1)

    with scope("picks"):
        loop(samples, find)
    with scope("fwdA"):
        settle(sib_a, group_sem.at[1])
    with scope("xA"):
        early(x_mine, arr_a)
        early(x_sib, sib_a)
    with scope("w1wait"):
        settle(w1, load_sem.at[1])
        for copy in small[4:]:
            copy.wait()
    with scope("upA"):
        over_rows(mine_part)
        over_rows(sib_part)
    with scope("w2wait"):
        settle(w2, load_sem.at[2])
    project(0)
    arrive(first, groups)
    with scope("xBm"):
        late(x_mine, arr_a, arr_b)
    with scope("upBm"):
        over_rows(mine_part)
    with scope("fwdB"):
        settle(sib_b, group_sem.at[2])
    with scope("xBs"):
        late(x_sib, sib_a, sib_b)
    with scope("upBs"):
        over_rows(sib_part)
    project(1)
    for n, (lo, size) in enumerate(outs):
        with scope(f"pwait{n}"):
            settle(part_in[n], precv_sem.at[n])

        def finish(k):
            r = rank_s[k]
            rows = pl.ds(k * BLOCK if isinstance(k, int) else pl.multiple_of(k * BLOCK, BLOCK), BLOCK)
            both = keep[r, :, lo : lo + size].astype(jnp.float32) + part_in[n][r].astype(jnp.float32)
            out_v[rows, lo : lo + size] = (both + b2_v[lo : lo + size]).astype(jnp.bfloat16)

        with scope(f"finish{n}"):
            loop(samples, finish)
    with scope("drain"):
        settle(arr_a, send_sem.at[2])
        settle(arr_b, send_sem.at[3])
        settle(outgo.at[1:], send_sem.at[0])
        settle(routes.at[1:], send_sem.at[1])
        for n in range(parts):
            settle(part_out[n], psend_sem.at[n])


def shards(encoded, counts, win_ids, dest_seq, dest_slot, w_first, b_first, w_second, b_second):
    samples, cap = win_ids.shape
    feat = encoded.shape[1]
    groups = lax.axis_size("dp")
    hid = w_first.shape[1]
    half_out = b_second.shape[0]
    rows = samples * BLOCK
    tile = rows // 2
    block_rows = BLOCK * feat // LANES
    outs = col_chunks(0, half_out, WIDE)
    parts = len(outs)
    late = samples // 2
    first = groups - late
    hbm = pl.BlockSpec(memory_space=pltpu.HBM)
    bf16, f32, i32 = jnp.bfloat16, jnp.float32, jnp.int32
    vmem, smem, dma = pltpu.VMEM, pltpu.SMEM, pltpu.SemaphoreType.DMA
    return pl.pallas_call(
        functools.partial(kernel, (groups, samples, cap, feat, parts)),
        out_shape=vmem((rows, half_out), bf16),
        in_specs=[hbm] * 9,
        out_specs=pl.BlockSpec(memory_space=pltpu.VMEM),
        scratch_shapes=[
            smem((samples,), i32), smem((samples,), i32), smem((samples,), i32),
            vmem((samples, cap), i32), vmem((hid,), f32), vmem((half_out,), f32),
            smem((2 * groups,), i32), smem((samples,), i32), smem((samples,), i32),
            vmem((feat, samples * cap), bf16),
            vmem((2, feat, hid), bf16),
            vmem((hid, 2 * half_out), bf16),
            vmem((samples, block_rows, LANES), bf16),
            vmem((groups, block_rows, LANES), bf16),
            vmem((first, block_rows, LANES), bf16),
            vmem((late, block_rows, LANES), bf16),
            vmem((first, block_rows, LANES), bf16),
            vmem((late, block_rows, LANES), bf16),
            vmem((1, LANES), i32),
            vmem((groups, 1, LANES), i32),
            vmem((tile, feat), bf16),
            vmem((tile, feat), bf16),
            vmem((tile, hid), f32),
            vmem((tile, hid), bf16),
            vmem((samples, BLOCK, half_out), bf16),
            *[vmem((samples, BLOCK, size), bf16) for _, size in outs],
            *[vmem((samples, BLOCK, size), bf16) for _, size in outs],
            pltpu.SemaphoreType.REGULAR((1,)), dma((6,)), dma((3,)), dma((4,)), dma((groups // 2,)), dma((3,)), dma((parts,)), dma((parts,)),
        ],
        compiler_params=pltpu.CompilerParams(
            collective_id=0, has_side_effects=True, vmem_limit_bytes=60 * 1024 * 1024
        ),
    )(
        dest_seq, dest_slot, counts, win_ids, b_first, b_second, encoded.T, w_first, w_second,
    )


def solution(mesh):
    placed = (
        P("dp", "tensor"), P("dp"), P("dp", None), P("dp"), P("dp"),
        P(None, "tensor"), P("tensor"), P("tensor", None), P("tensor"),
    )
    return jax.shard_map(
        shards, mesh=mesh, in_specs=placed, out_specs=P("dp", "tensor"), check_vma=False
    )
```
